32 devices in a mesh: gz: 2 (over core), pa: 16 (over z, y, x).
Axes of the slice: x: 2, y: 2, z: 4, core: 2. Of those that a mesh axis runs over, the one named last changes fastest.
Arguments:
- velocity: float32 [3, 2, 2, 512, 1024], P(None, 'gz', None, 'pa'), may hold values from -3 to 3
- mode_mask: int32 [512, 1024], P('pa'), may hold values from 0 to 1, as said below
Outputs:
- velocity_next: float32 [3, 2, 2, 512, 1024], P(None, 'gz', None, 'pa')
- divergence: float32 [2, 2, 512, 1024], P('gz', None, 'pa')
The draws below stay inside these ranges and needn't reach their ends.
Inputs may be any that keep to these rules, and one draw needn't show every extreme that they name: mode_mask is 1 exactly where |s(m)| <= A and n <= B, for one A from 256 to 340 and one B from 256 to 340 in each draw, and 0 elsewhere.
All inputs are finite; a program needn't handle non-finite values.
Results may differ from the reference program's by a relative error of at most 0.00005.
Values sent between devices are 32-bit elements; how exact they have to be, the bound alone decides.
A program may use at most 64 MiB of HBM per device.

```python
import math
import jax
import jax.numpy as jnp
from jax import lax

NX = 1024
NY = 1024
NZ = 2
KY = 512


def draw_mode_mask(key, part):
    first_key = jax.random.fold_in(key, 11)
    second_key = jax.random.fold_in(key, 23)
    cut_x = jax.random.randint(first_key, (), NX // 4, NX // 3)
    cut_y = jax.random.randint(second_key, (), NY // 4, NY // 3)
    modes = jnp.arange(NX, dtype=jnp.int32)
    signed = jnp.where(modes < NX // 2, modes, modes - NX)
    spanwise = jnp.arange(NY // 2, dtype=jnp.int32)
    inside = (jnp.abs(signed)[None, :] <= cut_x) & (spanwise[:, None] <= cut_y)
    return inside.astype(jnp.int32)


def shard_levels(stream_key, dims, shards, low, high):
    gain = 1.0
    for position, blocks in shards:
        steps = jax.random.uniform(jax.random.fold_in(jax.random.fold_in(stream_key, 6), position), (blocks,), jnp.float32, low / len(shards), high / len(shards))
        gain = gain * jnp.repeat(jnp.exp(steps), dims[position] // blocks).reshape((-1,) + (1,) * (len(dims) - 1 - position))
    return gain


def gaussian(key, shape, width, limit, shards=(), kind=jnp.bfloat16):
    factor_of = shard_levels(key, shape, shards, -0.22, 0.18) if shards else 1.0
    drawn = jax.random.normal(key, shape, jnp.float32) * width * factor_of
    return jnp.minimum(jnp.maximum(drawn, -limit), limit).astype(kind)


def setup_inputs(seed: int = 0) -> dict:
    keys = jax.random.split(jax.random.key(seed), 3)
    velocity = gaussian(keys[0], (3, NZ, 2, KY, NX), 0.5, 3.0, ((1, 2), (3, 16)), jnp.float32)
    mode_mask = draw_mode_mask(jax.random.fold_in(keys[2], 71), 0)
    return dict(velocity=velocity, mode_mask=mode_mask)


def wall_first(padded):
    return 0.5 * (padded[2:] - padded[:-2])


def times_wave(wave, field):
    return jnp.stack([-wave * field[:, 1], wave * field[:, 0]], 1)


def reference(velocity, mode_mask):
    half = NY // 2
    modes = jnp.arange(NX, dtype=jnp.int32)
    signed = jnp.where(modes < NX // 2, modes, modes - NX)
    kx_wave = (2.0 * math.pi / NX) * signed.astype(jnp.float32)
    ky_wave = ((2.0 * math.pi / NY) * jnp.arange(half, dtype=jnp.int32).astype(jnp.float32))[:, None]
    padded = jnp.pad(velocity, ((0, 0), (1, 1), (0, 0), (0, 0), (0, 0)))
    u_spec, v_spec, w_spec = velocity[0], velocity[1], velocity[2]
    omega_x = times_wave(ky_wave, w_spec) - wall_first(padded[1])
    omega_y = wall_first(padded[0]) - times_wave(kx_wave, w_spec)
    omega_z = times_wave(kx_wave, v_spec) - times_wave(ky_wave, u_spec)
    spectral = jnp.concatenate([velocity, jnp.stack([omega_x, omega_y, omega_z], 0)], 0)

    def plane(spec):
        coeff = spec[:, 0] + 1j * spec[:, 1]
        columns = jnp.fft.ifft(coeff, axis=2, norm="ortho")
        full = jnp.concatenate([columns, jnp.zeros((6, 1, NX), columns.dtype)], axis=1)
        grid = jnp.fft.irfft(full, n=NY, axis=1, norm="ortho")
        u_grid, v_grid, w_grid, ox_grid, oy_grid, oz_grid = grid[0], grid[1], grid[2], grid[3], grid[4], grid[5]
        cross = jnp.stack([v_grid * oz_grid - w_grid * oy_grid,
                           w_grid * ox_grid - u_grid * oz_grid,
                           u_grid * oy_grid - v_grid * ox_grid], 0)
        rows = jnp.fft.rfft(cross, axis=1, norm="ortho")[:, :half]
        result = jnp.fft.fft(rows, axis=2, norm="ortho")
        return jnp.stack([result.real, result.imag], 1)

    nonlinear = lax.map(plane, jnp.moveaxis(spectral, 1, 0))
    nonlinear = jnp.moveaxis(nonlinear, 0, 1)
    mask = mode_mask.astype(jnp.float32)
    viscous = padded[:, 2:] - 2.0 * padded[:, 1:-1] + padded[:, :-2]
    viscous = viscous - (kx_wave * kx_wave + ky_wave * ky_wave) * velocity
    following = velocity + 0.2 * (nonlinear * mask + 0.25 * viscous)
    w_padded = jnp.pad(following[2], ((1, 1), (0, 0), (0, 0), (0, 0)))
    divergence = times_wave(kx_wave, following[0]) + times_wave(ky_wave, following[1]) + wall_first(w_padded)
    return following, divergence
```

```python
import functools
import math

import jax
import jax.numpy as jnp
import numpy as np
from jax import lax
from jax.experimental import pallas as pl
from jax.experimental.pallas import tpu as pltpu
from jax.sharding import PartitionSpec as P

precise = lax.Precision.HIGHEST
time_step = 0.2
viscosity = 0.25


def extended(block, sides, width):
    for axis, dim in sides:
        count = lax.axis_size(axis)
        forward = [(i, i + 1) for i in range(count - 1)]
        backward = [(target, source) for source, target in forward]
        low = lax.ppermute(
            lax.slice_in_dim(block, block.shape[dim] - width, None, axis=dim), axis, forward
        )
        high = lax.ppermute(lax.slice_in_dim(block, 0, width, axis=dim), axis, backward)
        block = jnp.concatenate([low, block, high], axis=dim)
    return block


def phase_pair(rows, cols, period, sign):
    angle = 2.0 * math.pi / period * (rows[:, None] * cols[None, :] % period).astype(jnp.float32)
    return (jnp.cos(angle), sign * jnp.sin(angle))


def factor_sizes(length):
    second = 2 ** ((length.bit_length() - 1) // 2)
    return (length // second, second)


def factored(real, imag, sign, first, second, keep):
    used = real.shape[-1] // second
    lead = real.shape[:-1]
    a_index = jnp.arange(used, dtype=jnp.int32)
    c_index = jnp.arange(first, dtype=jnp.int32)
    b_index = jnp.arange(second, dtype=jnp.int32)
    d_index = jnp.arange(keep, dtype=jnp.int32)
    one_cos, one_sin = phase_pair(a_index, c_index, first, sign)
    turn_cos, turn_sin = phase_pair(c_index, b_index, first * second, sign)
    two_cos, two_sin = phase_pair(b_index, d_index, second, sign)
    x_real = real.reshape(lead + (used, second))
    a_real = jnp.einsum("...ab,ac->...cb", x_real, one_cos, precision=precise)
    a_imag = jnp.einsum("...ab,ac->...cb", x_real, one_sin, precision=precise)
    if imag is not None:
        x_imag = imag.reshape(lead + (used, second))
        a_real = a_real - jnp.einsum("...ab,ac->...cb", x_imag, one_sin, precision=precise)
        a_imag = a_imag + jnp.einsum("...ab,ac->...cb", x_imag, one_cos, precision=precise)
    t_real = a_real * turn_cos - a_imag * turn_sin
    t_imag = a_real * turn_sin + a_imag * turn_cos
    o_real = jnp.einsum("...cb,bd->...dc", t_real, two_cos, precision=precise) - jnp.einsum(
        "...cb,bd->...dc", t_imag, two_sin, precision=precise
    )
    o_imag = jnp.einsum("...cb,bd->...dc", t_real, two_sin, precision=precise) + jnp.einsum(
        "...cb,bd->...dc", t_imag, two_cos, precision=precise
    )
    return (o_real.reshape(lead + (keep * first,)), o_imag.reshape(lead + (keep * first,)))


def wall_first(padded):
    return 0.5 * (padded[2:] - padded[:-2])


def times_wave(wave, field):
    return jnp.stack([-wave * field[:, 1], wave * field[:, 0]], 1)


def by_steps(velocity, mode_mask):
    groups = lax.axis_size("pa")
    rank = lax.axis_index("pa")
    depth = velocity.shape[1]
    kyl = velocity.shape[3]
    ncols = velocity.shape[4]
    lines = ncols // groups
    half = kyl * groups
    nrows = 2 * half
    x_first, x_second = factor_sizes(ncols)
    y_first, y_second = factor_sizes(nrows)
    x_scale = 1.0 / math.sqrt(ncols)
    y_scale = 1.0 / math.sqrt(nrows)
    modes = jnp.arange(ncols, dtype=jnp.int32)
    signed = jnp.where(modes < ncols // 2, modes, modes - ncols)
    kx_wave = 2.0 * math.pi / ncols * signed.astype(jnp.float32)
    own_modes = rank * kyl + jnp.arange(kyl, dtype=jnp.int32)
    ky_wave = (2.0 * math.pi / nrows * own_modes.astype(jnp.float32))[:, None]
    span_index = jnp.arange(half, dtype=jnp.int32)
    weight = jnp.where(span_index == 0, 1.0, 2.0).astype(jnp.float32)

    def to_modes(received):
        count = received.shape[0]
        planes = received.shape[1]
        blocks = received.reshape(count, planes, 2, groups, lines, kyl)
        blocks = jnp.transpose(blocks, (0, 1, 2, 5, 3, 4)).reshape(count, planes, 2, kyl, ncols)
        h_real, h_imag = factored(
            blocks[:, :, 0], blocks[:, :, 1], -1.0, x_first, x_second, x_second
        )
        return jnp.stack([h_real, h_imag], 2) * x_scale

    padded = extended(velocity, (("gz", 1),), 1)
    u_spec = velocity[0]
    v_spec = velocity[1]
    w_spec = velocity[2]
    omega_x = times_wave(ky_wave, w_spec) - wall_first(padded[1])
    omega_y = wall_first(padded[0]) - times_wave(kx_wave, w_spec)
    omega_z = times_wave(kx_wave, v_spec) - times_wave(ky_wave, u_spec)
    vorticity = jnp.stack([omega_x, omega_y, omega_z], 0)
    both = jnp.concatenate([velocity, vorticity], 0)
    count = both.shape[0]
    g_real, g_imag = factored(both[:, :, 0], both[:, :, 1], 1.0, x_first, x_second, x_second)
    joined = jnp.stack([g_real, g_imag], 2) * x_scale
    joined = jnp.swapaxes(joined, 3, 4)
    received = lax.all_to_all(
        joined.reshape(count, depth, 2, groups, lines * kyl),
        "pa",
        split_axis=3,
        concat_axis=3,
        tiled=True,
    )
    to_count = received.shape[0]
    planes = received.shape[1]
    blocks = received.reshape(to_count, planes, 2, groups, lines, kyl)
    blocks = jnp.transpose(blocks, (0, 1, 2, 4, 3, 5)).reshape(to_count, planes, 2, lines, half)
    blocks = blocks * weight
    p_real, p_imag = factored(blocks[:, :, 0], blocks[:, :, 1], 1.0, y_first, y_second, y_second)
    grid = p_real * y_scale
    speed_grid = grid[:3]
    swirl_grid = grid[3:]
    u_grid = speed_grid[0]
    v_grid = speed_grid[1]
    w_grid = speed_grid[2]
    cross = jnp.stack(
        [
            v_grid * swirl_grid[2] - w_grid * swirl_grid[1],
            w_grid * swirl_grid[0] - u_grid * swirl_grid[2],
            u_grid * swirl_grid[1] - v_grid * swirl_grid[0],
        ],
        0,
    )
    count = cross.shape[0]
    q_real, q_imag = factored(cross, None, -1.0, y_first, y_second, y_second // 2)
    joined = jnp.stack([q_real, q_imag], 2) * y_scale
    joined = joined.reshape(count, depth, 2, lines, groups, kyl)
    joined = jnp.transpose(joined, (0, 1, 2, 4, 3, 5))
    nonlinear = to_modes(
        lax.all_to_all(
            joined.reshape(count, depth, 2, groups, lines * kyl),
            "pa",
            split_axis=3,
            concat_axis=3,
            tiled=True,
        )
    )
    mask = mode_mask.astype(jnp.float32)
    viscous = padded[:, 2:] - 2.0 * padded[:, 1:-1] + padded[:, :-2]
    viscous = viscous - (kx_wave * kx_wave + ky_wave * ky_wave) * velocity
    following = velocity + time_step * (nonlinear * mask + viscosity * viscous)
    w_padded = extended(following[2], (("gz", 0),), 1)
    divergence = (
        times_wave(kx_wave, following[0]) + times_wave(ky_wave, following[1]) + wall_first(w_padded)
    )
    return (following, divergence)


LANES = 128


def split(value):
    high = value.astype(jnp.bfloat16)
    low = (value - high.astype(jnp.float32)).astype(jnp.bfloat16)
    return high, low


def dot3(left, right):
    def dot(a, b):
        return jnp.dot(a, b, preferred_element_type=jnp.float32)

    return dot(left[0], right[0]) + (dot(left[0], right[1]) + dot(left[1], right[0]))


def turned(z, k, n, sign):
    real, imag = z
    if k == 0:
        return z
    if 4 * k == n:
        return (-imag, real) if sign > 0 else (imag, -real)
    c = math.cos(2.0 * math.pi * k / n)
    s = sign * math.sin(2.0 * math.pi * k / n)
    return (real * c - imag * s, real * s + imag * c)


def short_fft(z, sign):
    n = len(z)
    if n == 1:
        return z
    even = short_fft(z[0::2], sign)
    odd = short_fft(z[1::2], sign)
    low, high = [], []
    for k in range(n // 2):
        t = turned(odd[k], k, n, sign)
        low.append((even[k][0] + t[0], even[k][1] + t[1]))
        high.append((even[k][0] - t[0], even[k][1] - t[1]))
    return low + high


@functools.lru_cache(None)
def tables(ncols, nrows, lines):
    radix = ncols // LANES
    quarter = nrows // 4
    b = np.arange(LANES)
    angle = 2.0 * np.pi * (np.outer(b, b) % LANES) / LANES
    c, s = np.cos(angle), np.sin(angle)
    order = np.concatenate(
        [p * LANES + h * lines + np.arange(lines) for h in range(LANES // lines) for p in (0, 1)]
    )
    to_grid = np.block([[c, s], [-s, c]])[:, order] / math.sqrt(ncols)
    to_wave = np.block([[c, -s], [s, c]])[order, :] / math.sqrt(ncols) / 2.0
    q = np.arange(quarter)
    angle = 2.0 * np.pi * (np.outer(q, q) % quarter) / quarter
    span = np.concatenate([np.cos(angle), -np.sin(angle)], 1) * (2.0 / math.sqrt(nrows))
    angle = 2.0 * np.pi * np.outer(q, np.arange(4)) / nrows
    span_turn = np.concatenate([np.cos(angle), np.sin(angle)], 1)
    angle = 2.0 * np.pi * np.outer(np.arange(radix), b) / ncols
    line_turn = np.concatenate([np.cos(angle), np.sin(angle)], 0)
    return [np.asarray(t, np.float32) for t in (to_grid, to_wave, span, span_turn, line_turn)]


field_batches = ((0, 2), (2, 2), (4, 1))
back_batches = ((0, 1), (1, 2))


def kernel(
    groups, kept,
    vel_hbm, mask_hbm, to_grid_hbm, to_wave_hbm, span_hbm, span_turn_hbm, line_turn_hbm, kx_hbm,
    out, div,
    vel, mask, to_grid, to_wave, span, span_turn, line_turn, kx_ref,
    send, recv, vel_other, g_other, q_send, q_recv, w_other, grid,
    load_sem, send_sem, recv_sem, q_send_sem, q_recv_sem, pair_sem, pair_recv_sem,
):
    me = lax.axis_index("pa")
    side = lax.axis_index("gz")
    partner = {"gz": 1 - side}
    kyl = vel.shape[3]
    ncols = vel.shape[4]
    lines = ncols // groups
    half = kyl * groups
    nrows = 2 * half
    quarter = half // 2
    radix = ncols // LANES
    dz = jnp.where(side == 0, 0.5, -0.5).astype(jnp.float32)

    loads = {}
    for index, (name, src, dst) in enumerate(
        (
            ("v", vel_hbm.at[1], vel.at[1]),
            ("to_grid", to_grid_hbm, to_grid),
            ("line_turn", line_turn_hbm, line_turn),
            ("u", vel_hbm.at[0], vel.at[0]),
            ("w", vel_hbm.at[2], vel.at[2]),
            ("kx", kx_hbm, kx_ref),
            ("span", span_hbm, span),
            ("span_turn", span_turn_hbm, span_turn),
            ("to_wave", to_wave_hbm, to_wave),
            ("mask", mask_hbm, mask),
        )
    ):
        loads[name] = pltpu.make_async_copy(src, dst, load_sem.at[index])
        loads[name].start()

    barrier = pltpu.get_barrier_semaphore()

    @pl.loop(1, groups)
    def _(k):
        pl.semaphore_signal(barrier, inc=1, device_id={"pa": lax.rem(me + k, groups)})

    pl.semaphore_signal(barrier, inc=1, device_id=partner)

    own_n = me * kyl + lax.broadcasted_iota(jnp.int32, (kyl, LANES), 0)
    ky_own = 2.0 * math.pi / nrows * own_n.astype(jnp.float32)
    weight = jnp.where(own_n == 0, 0.5, 1.0).astype(jnp.float32)
    loads["v"].wait()
    loads["to_grid"].wait()
    loads["line_turn"].wait()
    grid_w = split(to_grid[...])

    def block(ref, a):
        return ref[:, a * LANES : (a + 1) * LANES]

    def kx_at(a):
        return jnp.broadcast_to(kx_ref[:, a * LANES : (a + 1) * LANES], (kyl, LANES))

    def spec(comp, a):
        at = slice(a * LANES, (a + 1) * LANES)
        return (vel[comp, 0, 0, :, at], vel[comp, 0, 1, :, at])

    def x_forward(slot, z):
        z = [(r * weight, i * weight) for r, i in z]
        lhs = []
        for c, (r, i) in enumerate(short_fft(z, 1.0)):
            if c > 0:
                tc = jnp.broadcast_to(line_turn[c : c + 1, :], (kyl, LANES))
                ts = jnp.broadcast_to(line_turn[radix + c : radix + c + 1, :], (kyl, LANES))
                r, i = r * tc - i * ts, r * ts + i * tc
            lhs.append(jnp.concatenate([r, i], 1))
        res = dot3(split(jnp.concatenate(lhs, 0)), grid_w)
        for c in range(radix):
            rows = res[c * kyl : (c + 1) * kyl]
            send[2 * c, slot] = rows[:, :LANES]
            send[2 * c + 1, slot] = rows[:, LANES:]

    def batch_copy(batch, dest, source):
        slots = pl.ds(*field_batches[batch])
        return pltpu.make_async_remote_copy(
            src_ref=send.at[dest, slots],
            dst_ref=recv.at[source, slots],
            send_sem=send_sem.at[batch, dest],
            recv_sem=recv_sem.at[batch, source],
            device_id={"pa": dest},
        )

    def send_batch(batch):
        @pl.loop(1, groups)
        def _(k):
            batch_copy(batch, lax.rem(me + k, groups), me).start()

        first_slot, count = field_batches[batch]
        for slot in range(first_slot, first_slot + count):
            recv[me, slot] = send[me, slot]

    def wait_batch(batch):
        @pl.loop(1, groups)
        def _(k):
            source = lax.rem(me + groups - k, groups)
            batch_copy(batch, source, source).wait_recv()

    def pair_copy(index, src, dst):
        return pltpu.make_async_remote_copy(
            src_ref=src,
            dst_ref=dst,
            send_sem=pair_sem.at[index],
            recv_sem=pair_recv_sem.at[index],
            device_id=partner,
        )

    x_forward(0, [spec(1, a) for a in range(radix)])
    loads["u"].wait()
    x_forward(1, [spec(0, a) for a in range(radix)])
    loads["w"].wait()
    loads["kx"].wait()
    pl.semaphore_wait(barrier, groups)
    send_batch(0)
    vel_copies = [pair_copy(f, vel.at[f, 0], vel_other.at[f]) for f in range(3)]
    for copy in vel_copies:
        copy.start()
    x_forward(2, [spec(2, a) for a in range(radix)])
    vel_copies[0].wait_recv()
    swirl = []
    for a in range(radix):
        w, kx = spec(2, a), kx_at(a)
        at = slice(a * LANES, (a + 1) * LANES)
        swirl.append((dz * vel_other[0, 0, :, at] + kx * w[1], dz * vel_other[0, 1, :, at] - kx * w[0]))
    x_forward(3, swirl)
    send_batch(1)
    swirl = []
    for a in range(radix):
        v, u, kx = spec(1, a), spec(0, a), kx_at(a)
        swirl.append((ky_own * u[1] - kx * v[1], kx * v[0] - ky_own * u[0]))
    x_forward(4, swirl)
    send_batch(2)

    vel_copies[1].wait_recv()
    vel_copies[2].wait_recv()
    ky_wide = ky_own[:, :1]
    square = kx_ref[...] * kx_ref[...] + ky_wide * ky_wide
    for f in range(3):
        for part in range(2):
            own = vel[f, 0, part]
            viscous = vel_other[f, part] - 2.0 * own - square * own
            out[f, 0, part] = own + time_step * viscosity * viscous

    loads["span"].wait()
    loads["span_turn"].wait()
    span_w = split(span[...])
    lane = lax.broadcasted_iota(jnp.int32, (half, LANES), 1)
    first = lane < lines
    all_n = lax.broadcasted_iota(jnp.int32, (half, LANES), 0)
    ky_all = 2.0 * math.pi / nrows * all_n.astype(jnp.float32)
    ky_all = jnp.where(first, -ky_all, ky_all)

    def swap(value):
        return pltpu.roll(value, lines, 1)

    def turn(t):
        c = jnp.broadcast_to(span_turn[:, t : t + 1], (quarter, LANES))
        s = jnp.broadcast_to(span_turn[:, 4 + t : 5 + t], (quarter, LANES))
        return c, s

    def field(slot):
        return recv[:, slot].reshape(half, LANES)

    def y_forward(pair, one, two):
        real = jnp.where(first, one, swap(two))
        imag = jnp.where(first, swap(one), two)
        rl, rh, il, ih = real[:quarter], real[quarter:], imag[:quarter], imag[quarter:]
        columns = []
        for t, (r, i) in enumerate(
            [(rl + rh, il + ih), (rl - ih, il + rh), (rl - rh, il - ih), (rl + ih, il - rh)]
        ):
            if t > 0:
                c, s = turn(t)
                r, i = r * c - i * s, r * s + i * c
            columns.append(jnp.concatenate([r, i], 0))
        res = dot3(span_w, split(jnp.concatenate(columns, 1)))
        for t in range(4):
            grid[pair, t] = res[:, t * LANES : (t + 1) * LANES]

    back_w = span[...]
    back_w = split(jnp.concatenate([back_w[:, :quarter], back_w[:, quarter:]], 0))
    lo = lax.broadcasted_iota(jnp.int32, (quarter, LANES), 1) < lines

    def q_copy(batch, dest, source):
        slots = pl.ds(*back_batches[batch])
        return pltpu.make_async_remote_copy(
            src_ref=q_send.at[dest, slots],
            dst_ref=q_recv.at[source, slots],
            send_sem=q_send_sem.at[batch, dest],
            recv_sem=q_recv_sem.at[batch, source],
            device_id={"pa": dest},
        )

    def q_start(batch):
        @pl.loop(1, groups)
        def _(k):
            dest = lax.rem(me + k, groups)

            @pl.when(dest < kept)
            def _():
                q_copy(batch, dest, me).start()

        first_slot, count = back_batches[batch]
        for slot in range(first_slot, first_slot + count):
            q_recv[me, slot] = q_send[me, slot]

    def q_wait(batch):
        @pl.loop(1, groups)
        def _(k):
            source = lax.rem(me + groups - k, groups)
            q_copy(batch, source, source).wait_recv()

    def y_back(columns, comps):
        res = dot3(back_w, split(jnp.concatenate(columns, 1)))
        sums = []
        for t in range(4):
            r = res[:quarter, t * LANES : (t + 1) * LANES]
            i = res[quarter:, t * LANES : (t + 1) * LANES]
            if t > 0:
                c, s = turn(t)
                r, i = r * c + i * s, i * c - r * s
            sums.append((r, i))
        (r0, i0), (r1, i1), (r2, i2), (r3, i3) = sums
        low = (r0 + r1 + r2 + r3, i0 + i1 + i2 + i3)
        high = (r0 - r2 + (i1 - i3), i0 - i2 - (r1 - r3))
        for base, (r, i), count in (
            (0, low, quarter // kyl),
            (quarter // kyl, high, kept - quarter // kyl),
        ):
            rolled_i, rolled_r = swap(i), swap(r)
            packed = [jnp.where(lo, r, rolled_i), jnp.where(lo, rolled_r, i)]
            for comp, value in zip(comps, packed):
                q_send[base : base + count, comp] = value[: count * kyl].reshape(count, kyl, LANES)

    wait_batch(0)
    v_copy = pair_copy(3, recv.at[:, 0], g_other)
    v_copy.start()
    y_forward(0, field(1), field(0))
    wait_batch(1)
    v_copy.wait_recv()
    swirl_x = ky_all * swap(field(2)) - dz * g_other[...].reshape(half, LANES)
    y_forward(1, field(3), swirl_x)
    columns = []
    for t in range(4):
        product = grid[0, t] * grid[1, t]
        columns.append(product - swap(product))
    y_back(columns, (0,))
    q_start(0)
    wait_batch(2)
    y_forward(2, field(2), field(4))
    columns = []
    for t in range(4):
        speed, swirls, mixed = grid[0, t], grid[1, t], grid[2, t]
        x_part = swap(speed * mixed) - mixed * swirls
        y_part = mixed * swap(swirls) - speed * swap(mixed)
        columns.append(jnp.where(lo, x_part, swap(y_part)))
    y_back(columns, (1, 2))
    q_start(1)

    loads["to_wave"].wait()
    loads["mask"].wait()
    wave_w = split(to_wave[...])

    def x_back(slot, comp):
        rows = [
            jnp.concatenate([q_recv[2 * c, slot], q_recv[2 * c + 1, slot]], 1)
            for c in range(radix)
        ]
        res = dot3(split(jnp.concatenate(rows, 0)), wave_w)
        z = []
        for c in range(radix):
            r = res[c * kyl : (c + 1) * kyl, :LANES]
            i = res[c * kyl : (c + 1) * kyl, LANES:]
            if c > 0:
                tc = jnp.broadcast_to(line_turn[c : c + 1, :], (kyl, LANES))
                ts = jnp.broadcast_to(line_turn[radix + c : radix + c + 1, :], (kyl, LANES))
                r, i = r * tc + i * ts, i * tc - r * ts
            z.append((r, i))
        for a, values in enumerate(short_fft(z, -1.0)):
            at = slice(a * LANES, (a + 1) * LANES)
            gain = time_step * mask[:, at].astype(jnp.float32)
            for part in range(2):
                out[comp, 0, part, :, at] = out[comp, 0, part, :, at] + gain * values[part]

    @pl.when(me < kept)
    def _():
        q_wait(0)
        x_back(0, 2)

    w_copy = pair_copy(4, out.at[2, 0], w_other)
    w_copy.start()

    @pl.when(me < kept)
    def _():
        q_wait(1)
        x_back(1, 0)
        x_back(2, 1)

    kx_all = kx_ref[...]
    w_copy.wait_recv()
    for part, sign in ((0, -1.0), (1, 1.0)):
        u_next = out[0, 0, 1 - part]
        v_next = out[1, 0, 1 - part]
        div[0, part] = dz * w_other[part] + sign * (kx_all * u_next + ky_wide * v_next)

    for copy in vel_copies + [v_copy, w_copy]:
        copy.wait_send()

    for batch in range(len(field_batches)):

        @pl.loop(1, groups)
        def _(k):
            batch_copy(batch, lax.rem(me + k, groups), me).wait_send()

    for batch in range(len(back_batches)):

        @pl.loop(1, groups)
        def _(k):
            dest = lax.rem(me + k, groups)

            @pl.when(dest < kept)
            def _():
                q_copy(batch, dest, me).wait_send()


def store_kernel(next_ref, div_ref, next_out, div_out, sem):
    copies = [pltpu.make_async_copy(next_ref.at[f], next_out.at[f], sem.at[f]) for f in range(3)]
    copies.append(pltpu.make_async_copy(div_ref, div_out, sem.at[3]))
    for copy in copies:
        copy.start()
    for copy in copies:
        copy.wait()


def in_one_kernel(velocity, mode_mask):
    groups = lax.axis_size("pa")
    kyl = velocity.shape[3]
    ncols = velocity.shape[4]
    lines = ncols // groups
    half = kyl * groups
    nrows = 2 * half
    kept = -(-(nrows // 3) // kyl)
    signed = np.where(np.arange(ncols) < ncols // 2, np.arange(ncols), np.arange(ncols) - ncols)
    kx = (np.float32(2.0 * math.pi / ncols) * signed.astype(np.float32))[None, :]
    operands = [velocity, mode_mask] + [jnp.asarray(t) for t in tables(ncols, nrows, lines)]
    operands.append(jnp.asarray(kx))
    f32 = jnp.float32
    hbm = pl.BlockSpec(memory_space=pltpu.HBM)
    whole = pl.BlockSpec(memory_space=pl.ANY)
    vmem = pl.BlockSpec(memory_space=pltpu.VMEM)
    dma = pltpu.SemaphoreType.DMA
    shapes = (
        jax.ShapeDtypeStruct(velocity.shape, f32),
        jax.ShapeDtypeStruct(velocity.shape[1:], f32),
    )
    following, divergence = pl.pallas_call(
        functools.partial(kernel, groups, kept),
        out_shape=shapes,
        in_specs=[hbm] * len(operands),
        out_specs=(vmem, vmem),
        scratch_shapes=[pltpu.VMEM(t.shape, t.dtype) for t in operands]
        + [
            pltpu.VMEM((groups, 5, kyl, LANES), f32),
            pltpu.VMEM((groups, 5, kyl, LANES), f32),
            pltpu.VMEM((3, 2, kyl, ncols), f32),
            pltpu.VMEM((groups, kyl, LANES), f32),
            pltpu.VMEM((groups, 3, kyl, LANES), f32),
            pltpu.VMEM((groups, 3, kyl, LANES), f32),
            pltpu.VMEM((2, kyl, ncols), f32),
            pltpu.VMEM((3, 4, half // 2, LANES), f32),
            dma((10,)),
            dma((len(field_batches), groups)),
            dma((len(field_batches), groups)),
            dma((len(back_batches), groups)),
            dma((len(back_batches), groups)),
            dma((5,)),
            dma((5,)),
        ],
        compiler_params=pltpu.CompilerParams(collective_id=0, has_side_effects=True, vmem_limit_bytes=32 * 2**20),
    )(*[pltpu.with_memory_space_constraint(x, pltpu.HBM) for x in operands])
    return pl.pallas_call(
        store_kernel,
        out_shape=shapes,
        in_specs=[whole, whole],
        out_specs=(hbm, hbm),
        scratch_shapes=[dma((4,))],
        compiler_params=pltpu.CompilerParams(vmem_limit_bytes=2**20),
    )(following, divergence)


def on_device(velocity, mode_mask):
    groups = lax.axis_size("pa")
    kyl = velocity.shape[3]
    ncols = velocity.shape[4]
    fits = (
        lax.axis_size("gz") == 2
        and velocity.shape[1] == 1
        and kyl % 8 == 0
        and 2 * (ncols // groups) == LANES
        and (kyl * groups // 2) % LANES == 0
        and ncols % LANES == 0
        and nrows_cover(kyl * groups)
    )
    return in_one_kernel(velocity, mode_mask) if fits else by_steps(velocity, mode_mask)


def nrows_cover(half):
    return 2 * half // 3 > half // 2


def solution(mesh):
    placed = (P(None, "gz", None, "pa", None), P("pa", None))
    return jax.shard_map(
        on_device,
        mesh=mesh,
        in_specs=placed,
        out_specs=(P(None, "gz", None, "pa", None), P("gz", None, "pa", None)),
        check_vma=False,
    )
```

```python
import functools
import math

import jax
import jax.numpy as jnp
import numpy as np
from jax import lax
from jax.experimental import pallas as pl
from jax.experimental.pallas import tpu as pltpu
from jax.sharding import PartitionSpec as P

precise = lax.Precision.HIGHEST
time_step = 0.2
viscosity = 0.25


def extended(block, sides, width):
    for axis, dim in sides:
        count = lax.axis_size(axis)
        forward = [(i, i + 1) for i in range(count - 1)]
        backward = [(target, source) for source, target in forward]
        low = lax.ppermute(
            lax.slice_in_dim(block, block.shape[dim] - width, None, axis=dim), axis, forward
        )
        high = lax.ppermute(lax.slice_in_dim(block, 0, width, axis=dim), axis, backward)
        block = jnp.concatenate([low, block, high], axis=dim)
    return block


def phase_pair(rows, cols, period, sign):
    angle = 2.0 * math.pi / period * (rows[:, None] * cols[None, :] % period).astype(jnp.float32)
    return (jnp.cos(angle), sign * jnp.sin(angle))


def factor_sizes(length):
    second = 2 ** ((length.bit_length() - 1) // 2)
    return (length // second, second)


def factored(real, imag, sign, first, second, keep):
    used = real.shape[-1] // second
    lead = real.shape[:-1]
    a_index = jnp.arange(used, dtype=jnp.int32)
    c_index = jnp.arange(first, dtype=jnp.int32)
    b_index = jnp.arange(second, dtype=jnp.int32)
    d_index = jnp.arange(keep, dtype=jnp.int32)
    one_cos, one_sin = phase_pair(a_index, c_index, first, sign)
    turn_cos, turn_sin = phase_pair(c_index, b_index, first * second, sign)
    two_cos, two_sin = phase_pair(b_index, d_index, second, sign)
    x_real = real.reshape(lead + (used, second))
    a_real = jnp.einsum("...ab,ac->...cb", x_real, one_cos, precision=precise)
    a_imag = jnp.einsum("...ab,ac->...cb", x_real, one_sin, precision=precise)
    if imag is not None:
        x_imag = imag.reshape(lead + (used, second))
        a_real = a_real - jnp.einsum("...ab,ac->...cb", x_imag, one_sin, precision=precise)
        a_imag = a_imag + jnp.einsum("...ab,ac->...cb", x_imag, one_cos, precision=precise)
    t_real = a_real * turn_cos - a_imag * turn_sin
    t_imag = a_real * turn_sin + a_imag * turn_cos
    o_real = jnp.einsum("...cb,bd->...dc", t_real, two_cos, precision=precise) - jnp.einsum(
        "...cb,bd->...dc", t_imag, two_sin, precision=precise
    )
    o_imag = jnp.einsum("...cb,bd->...dc", t_real, two_sin, precision=precise) + jnp.einsum(
        "...cb,bd->...dc", t_imag, two_cos, precision=precise
    )
    return (o_real.reshape(lead + (keep * first,)), o_imag.reshape(lead + (keep * first,)))


def wall_first(padded):
    return 0.5 * (padded[2:] - padded[:-2])


def times_wave(wave, field):
    return jnp.stack([-wave * field[:, 1], wave * field[:, 0]], 1)


def by_steps(velocity, mode_mask):
    groups = lax.axis_size("pa")
    rank = lax.axis_index("pa")
    depth = velocity.shape[1]
    kyl = velocity.shape[3]
    ncols = velocity.shape[4]
    lines = ncols // groups
    half = kyl * groups
    nrows = 2 * half
    x_first, x_second = factor_sizes(ncols)
    y_first, y_second = factor_sizes(nrows)
    x_scale = 1.0 / math.sqrt(ncols)
    y_scale = 1.0 / math.sqrt(nrows)
    modes = jnp.arange(ncols, dtype=jnp.int32)
    signed = jnp.where(modes < ncols // 2, modes, modes - ncols)
    kx_wave = 2.0 * math.pi / ncols * signed.astype(jnp.float32)
    own_modes = rank * kyl + jnp.arange(kyl, dtype=jnp.int32)
    ky_wave = (2.0 * math.pi / nrows * own_modes.astype(jnp.float32))[:, None]
    span_index = jnp.arange(half, dtype=jnp.int32)
    weight = jnp.where(span_index == 0, 1.0, 2.0).astype(jnp.float32)

    def to_modes(received):
        count = received.shape[0]
        planes = received.shape[1]
        blocks = received.reshape(count, planes, 2, groups, lines, kyl)
        blocks = jnp.transpose(blocks, (0, 1, 2, 5, 3, 4)).reshape(count, planes, 2, kyl, ncols)
        h_real, h_imag = factored(
            blocks[:, :, 0], blocks[:, :, 1], -1.0, x_first, x_second, x_second
        )
        return jnp.stack([h_real, h_imag], 2) * x_scale

    padded = extended(velocity, (("gz", 1),), 1)
    u_spec = velocity[0]
    v_spec = velocity[1]
    w_spec = velocity[2]
    omega_x = times_wave(ky_wave, w_spec) - wall_first(padded[1])
    omega_y = wall_first(padded[0]) - times_wave(kx_wave, w_spec)
    omega_z = times_wave(kx_wave, v_spec) - times_wave(ky_wave, u_spec)
    vorticity = jnp.stack([omega_x, omega_y, omega_z], 0)
    both = jnp.concatenate([velocity, vorticity], 0)
    count = both.shape[0]
    g_real, g_imag = factored(both[:, :, 0], both[:, :, 1], 1.0, x_first, x_second, x_second)
    joined = jnp.stack([g_real, g_imag], 2) * x_scale
    joined = jnp.swapaxes(joined, 3, 4)
    received = lax.all_to_all(
        joined.reshape(count, depth, 2, groups, lines * kyl),
        "pa",
        split_axis=3,
        concat_axis=3,
        tiled=True,
    )
    to_count = received.shape[0]
    planes = received.shape[1]
    blocks = received.reshape(to_count, planes, 2, groups, lines, kyl)
    blocks = jnp.transpose(blocks, (0, 1, 2, 4, 3, 5)).reshape(to_count, planes, 2, lines, half)
    blocks = blocks * weight
    p_real, p_imag = factored(blocks[:, :, 0], blocks[:, :, 1], 1.0, y_first, y_second, y_second)
    grid = p_real * y_scale
    speed_grid = grid[:3]
    swirl_grid = grid[3:]
    u_grid = speed_grid[0]
    v_grid = speed_grid[1]
    w_grid = speed_grid[2]
    cross = jnp.stack(
        [
            v_grid * swirl_grid[2] - w_grid * swirl_grid[1],
            w_grid * swirl_grid[0] - u_grid * swirl_grid[2],
            u_grid * swirl_grid[1] - v_grid * swirl_grid[0],
        ],
        0,
    )
    count = cross.shape[0]
    q_real, q_imag = factored(cross, None, -1.0, y_first, y_second, y_second // 2)
    joined = jnp.stack([q_real, q_imag], 2) * y_scale
    joined = joined.reshape(count, depth, 2, lines, groups, kyl)
    joined = jnp.transpose(joined, (0, 1, 2, 4, 3, 5))
    nonlinear = to_modes(
        lax.all_to_all(
            joined.reshape(count, depth, 2, groups, lines * kyl),
            "pa",
            split_axis=3,
            concat_axis=3,
            tiled=True,
        )
    )
    mask = mode_mask.astype(jnp.float32)
    viscous = padded[:, 2:] - 2.0 * padded[:, 1:-1] + padded[:, :-2]
    viscous = viscous - (kx_wave * kx_wave + ky_wave * ky_wave) * velocity
    following = velocity + time_step * (nonlinear * mask + viscosity * viscous)
    w_padded = extended(following[2], (("gz", 0),), 1)
    divergence = (
        times_wave(kx_wave, following[0]) + times_wave(ky_wave, following[1]) + wall_first(w_padded)
    )
    return (following, divergence)


LANES = 128


def split(value):
    high = value.astype(jnp.bfloat16)
    low = (value - high.astype(jnp.float32)).astype(jnp.bfloat16)
    return high, low


def dot3(left, right):
    def dot(a, b):
        return jnp.dot(a, b, preferred_element_type=jnp.float32)

    return dot(left[0], right[0]) + (dot(left[0], right[1]) + dot(left[1], right[0]))


def turned(z, k, n, sign):
    real, imag = z
    if k == 0:
        return z
    if 4 * k == n:
        return (-imag, real) if sign > 0 else (imag, -real)
    c = math.cos(2.0 * math.pi * k / n)
    s = sign * math.sin(2.0 * math.pi * k / n)
    return (real * c - imag * s, real * s + imag * c)


def short_fft(z, sign):
    n = len(z)
    if n == 1:
        return z
    even = short_fft(z[0::2], sign)
    odd = short_fft(z[1::2], sign)
    low, high = [], []
    for k in range(n // 2):
        t = turned(odd[k], k, n, sign)
        low.append((even[k][0] + t[0], even[k][1] + t[1]))
        high.append((even[k][0] - t[0], even[k][1] - t[1]))
    return low + high


@functools.lru_cache(None)
def tables(ncols, nrows, lines):
    radix = ncols // LANES
    quarter = nrows // 4
    b = np.arange(LANES)
    angle = 2.0 * np.pi * (np.outer(b, b) % LANES) / LANES
    c, s = np.cos(angle), np.sin(angle)
    order = np.concatenate(
        [p * LANES + h * lines + np.arange(lines) for h in range(LANES // lines) for p in (0, 1)]
    )
    to_grid = np.block([[c, s], [-s, c]])[:, order] / math.sqrt(ncols)
    to_wave = np.block([[c, -s], [s, c]])[order, :] / math.sqrt(ncols) / 2.0
    q = np.arange(quarter)
    angle = 2.0 * np.pi * (np.outer(q, q) % quarter) / quarter
    span = np.concatenate([np.cos(angle), -np.sin(angle)], 1) * (2.0 / math.sqrt(nrows))
    angle = 2.0 * np.pi * np.outer(q, np.arange(4)) / nrows
    span_turn = np.concatenate([np.cos(angle), np.sin(angle)], 1)
    angle = 2.0 * np.pi * np.outer(np.arange(radix), b) / ncols
    line_turn = np.concatenate([np.cos(angle), np.sin(angle)], 0)
    return [np.asarray(t, np.float32) for t in (to_grid, to_wave, span, span_turn, line_turn)]


PLANE = 4
NEAR = 1
field_batches = ((0, 2), (2, 2), (4, 1))
back_batches = ((0, 1), (1, 2))


def kernel(
    groups, kept,
    vel_hbm, mask_hbm, to_grid_hbm, to_wave_hbm, span_hbm, span_turn_hbm, line_turn_hbm, kx_hbm,
    out, div,
    vel, mask, to_grid, to_wave, span, span_turn, line_turn, kx_ref,
    send, recv, vel_other, g_other, q_send, q_recv, w_other, grid,
    load_sem, send_sem, recv_sem, q_send_sem, q_recv_sem, pair_sem, pair_recv_sem, ready,
    hop, hop_sem, hop_recv_sem, pass_sem,
):
    me = lax.axis_index("pa")
    side = lax.axis_index("gz")
    partner = {"gz": 1 - side}
    kyl = vel.shape[3]
    ncols = vel.shape[4]
    lines = ncols // groups
    half = kyl * groups
    nrows = 2 * half
    quarter = half // 2
    radix = ncols // LANES
    dz = jnp.where(side == 0, 0.5, -0.5).astype(jnp.float32)

    depth = groups // PLANE
    diameter = depth + 1
    layer = me // PLANE
    column = lax.rem(me, PLANE)
    flipped = [column]
    for step in (1, 2):
        flipped += [f + step - 2 * step * lax.rem(f // step, 2) for f in flipped]
    reach = sorted(range(1 - depth, depth), key=lambda d: (-abs(d), -d))

    def columns_within(shift, low, high):
        return [c for c in range(PLANE) if low <= abs(shift) + c.bit_count() <= high]

    def each_peer(low, high, act):
        for shift in reach:
            chosen = columns_within(shift, low, high)
            if not chosen:
                continue

            def visit(shift=shift, chosen=chosen):
                for c in chosen:
                    act((layer + shift) * PLANE + flipped[c])

            if shift == 0:
                visit()
            else:
                pl.when((layer + shift >= 0) & (layer + shift < depth))(visit)

    def peers(low, high):
        total = 0
        for shift in reach:
            count = len(columns_within(shift, low, high))
            inside = (layer + shift >= 0) & (layer + shift < depth)
            total = total + jnp.where(inside, count, 0)
        return total

    barrier = pltpu.get_barrier_semaphore()
    each_peer(1, NEAR, lambda d: pl.semaphore_signal(barrier, inc=1, device_id={"pa": d}))
    pl.semaphore_signal(barrier, inc=1, device_id=partner)

    loads = {}
    for index, (name, src, dst) in enumerate(
        (
            ("v", vel_hbm.at[1], vel.at[1]),
            ("to_grid", to_grid_hbm, to_grid),
            ("line_turn", line_turn_hbm, line_turn),
            ("u", vel_hbm.at[0], vel.at[0]),
            ("w", vel_hbm.at[2], vel.at[2]),
            ("kx", kx_hbm, kx_ref),
            ("span", span_hbm, span),
            ("span_turn", span_turn_hbm, span_turn),
            ("to_wave", to_wave_hbm, to_wave),
            ("mask", mask_hbm, mask),
        )
    ):
        loads[name] = pltpu.make_async_copy(src, dst, load_sem.at[index])
        loads[name].start()

    own_n = me * kyl + lax.broadcasted_iota(jnp.int32, (kyl, LANES), 0)
    ky_own = 2.0 * math.pi / nrows * own_n.astype(jnp.float32)
    weight = jnp.where(own_n == 0, 0.5, 1.0).astype(jnp.float32)
    loads["v"].wait()
    loads["to_grid"].wait()
    loads["line_turn"].wait()
    grid_w = split(to_grid[...])

    def block(ref, a):
        return ref[:, a * LANES : (a + 1) * LANES]

    def kx_at(a):
        return jnp.broadcast_to(kx_ref[:, a * LANES : (a + 1) * LANES], (kyl, LANES))

    def spec(comp, a):
        at = slice(a * LANES, (a + 1) * LANES)
        return (vel[comp, 0, 0, :, at], vel[comp, 0, 1, :, at])

    def x_forward(slot, z):
        z = [(r * weight, i * weight) for r, i in z]
        lhs = []
        for c, (r, i) in enumerate(short_fft(z, 1.0)):
            if c > 0:
                tc = jnp.broadcast_to(line_turn[c : c + 1, :], (kyl, LANES))
                ts = jnp.broadcast_to(line_turn[radix + c : radix + c + 1, :], (kyl, LANES))
                r, i = r * tc - i * ts, r * ts + i * tc
            lhs.append(jnp.concatenate([r, i], 1))
        res = dot3(split(jnp.concatenate(lhs, 0)), grid_w)
        for c in range(radix):
            rows = res[c * kyl : (c + 1) * kyl]
            send[2 * c, slot] = rows[:, :LANES]
            send[2 * c + 1, slot] = rows[:, LANES:]

    def batch_copy(batch, dest, source):
        slots = pl.ds(*field_batches[batch])
        return pltpu.make_async_remote_copy(
            src_ref=send.at[dest, slots],
            dst_ref=recv.at[source, slots],
            send_sem=send_sem.at[batch, dest],
            recv_sem=recv_sem.at[batch, source],
            device_id={"pa": dest},
        )

    def send_batch(batch):
        @pl.loop(1, groups)
        def _(k):
            batch_copy(batch, lax.rem(me + k, groups), me).start()

        keep_own(batch)

    def keep_own(batch):
        first_slot, count = field_batches[batch]
        for slot in range(first_slot, first_slot + count):
            recv[me, slot] = send[me, slot]

    def wait_batch(batch):
        @pl.loop(1, groups)
        def _(k):
            source = lax.rem(me + groups - k, groups)

            @pl.when((source != mate) | jnp.logical_not(middle) | (batch > 0))
            def _():
                batch_copy(batch, source, source).wait_recv()

    def pair_copy(index, src, dst):
        return pltpu.make_async_remote_copy(
            src_ref=src,
            dst_ref=dst,
            send_sem=pair_sem.at[index],
            recv_sem=pair_recv_sem.at[index],
            device_id=partner,
        )

    x_forward(0, [spec(1, a) for a in range(radix)])
    loads["u"].wait()
    x_forward(1, [spec(0, a) for a in range(radix)])
    loads["w"].wait()
    loads["kx"].wait()
    pl.semaphore_wait(barrier, peers(1, NEAR) + 1)

    half_depth = depth // 2
    upper = layer >= half_depth
    middle = (layer == half_depth) | (layer == half_depth - 1)
    mate = jnp.where(upper, me - PLANE, me + PLANE)
    own_half = jnp.where(upper, groups // 2, 0)
    other_half = groups // 2 - own_half
    lead = pl.ds(*field_batches[0])

    def hop_copy(index):
        return pltpu.make_async_remote_copy(
            src_ref=send.at[pl.ds(other_half + index * PLANE, PLANE), lead],
            dst_ref=hop.at[index],
            send_sem=hop_sem.at[index],
            recv_sem=hop_recv_sem.at[index],
            device_id={"pa": mate},
        )

    def pass_copy(index, c):
        return pltpu.make_async_remote_copy(
            src_ref=hop.at[index, c],
            dst_ref=recv.at[mate, lead],
            send_sem=pass_sem.at[index, c],
            recv_sem=recv_sem.at[0, mate],
            device_id={"pa": own_half + index * PLANE + c},
        )

    def each_pass(index, act):
        for c in range(PLANE):

            @pl.when(own_half + index * PLANE + c != me)
            def _():
                act(pass_copy(index, c))

    def pass_on():
        @pl.when(middle)
        def _():
            for index in range(half_depth):
                hop_copy(index).wait_recv()
                each_pass(index, lambda copy: copy.start())
                for c in range(PLANE):

                    @pl.when(own_half + index * PLANE + c == me)
                    def _():
                        recv[mate, lead] = hop[index, c]

    def direct(dest):
        return jnp.logical_not(middle & ((dest >= groups // 2) != upper))

    steps = []
    known = NEAR
    while known < diameter:
        steps.append(min(known, diameter - known))
        known += steps[-1]

    def tell(index):
        if index < len(steps):
            each_peer(
                1,
                steps[index],
                lambda d: pl.semaphore_signal(ready.at[index], inc=1, device_id={"pa": d}),
            )

    def hear(index):
        if index < len(steps):
            pl.semaphore_wait(ready.at[index], peers(1, steps[index]))
            tell(index + 1)

    tell(0)

    @pl.when(middle)
    def _():
        for index in range(half_depth):
            hop_copy(index).start()

    keep_own(0)
    vel_copies = [pair_copy(f, vel.at[f, 0], vel_other.at[f]) for f in range(3)]
    for copy in vel_copies:
        copy.start()
    x_forward(2, [spec(2, a) for a in range(radix)])
    hear(0)
    vel_copies[0].wait_recv()
    swirl = []
    for a in range(radix):
        w, kx = spec(2, a), kx_at(a)
        at = slice(a * LANES, (a + 1) * LANES)
        swirl.append((dz * vel_other[0, 0, :, at] + kx * w[1], dz * vel_other[0, 1, :, at] - kx * w[0]))
    x_forward(3, swirl)
    for index in range(1, len(steps)):
        hear(index)

    @pl.loop(1, groups)
    def _(k):
        dest = lax.rem(me + k, groups)

        @pl.when(direct(dest))
        def _():
            batch_copy(0, dest, me).start()

    send_batch(1)
    swirl = []
    for a in range(radix):
        v, u, kx = spec(1, a), spec(0, a), kx_at(a)
        swirl.append((ky_own * u[1] - kx * v[1], kx * v[0] - ky_own * u[0]))
    x_forward(4, swirl)
    send_batch(2)

    vel_copies[1].wait_recv()
    vel_copies[2].wait_recv()
    ky_wide = ky_own[:, :1]
    square = kx_ref[...] * kx_ref[...] + ky_wide * ky_wide
    for f in range(3):
        for part in range(2):
            own = vel[f, 0, part]
            viscous = vel_other[f, part] - 2.0 * own - square * own
            out[f, 0, part] = own + time_step * viscosity * viscous

    loads["span"].wait()
    loads["span_turn"].wait()
    span_w = split(span[...])
    lane = lax.broadcasted_iota(jnp.int32, (half, LANES), 1)
    first = lane < lines
    all_n = lax.broadcasted_iota(jnp.int32, (half, LANES), 0)
    ky_all = 2.0 * math.pi / nrows * all_n.astype(jnp.float32)
    ky_all = jnp.where(first, -ky_all, ky_all)

    def swap(value):
        return pltpu.roll(value, lines, 1)

    def turn(t):
        c = jnp.broadcast_to(span_turn[:, t : t + 1], (quarter, LANES))
        s = jnp.broadcast_to(span_turn[:, 4 + t : 5 + t], (quarter, LANES))
        return c, s

    def field(slot):
        return recv[:, slot].reshape(half, LANES)

    def y_forward(pair, one, two):
        real = jnp.where(first, one, swap(two))
        imag = jnp.where(first, swap(one), two)
        rl, rh, il, ih = real[:quarter], real[quarter:], imag[:quarter], imag[quarter:]
        columns = []
        for t, (r, i) in enumerate(
            [(rl + rh, il + ih), (rl - ih, il + rh), (rl - rh, il - ih), (rl + ih, il - rh)]
        ):
            if t > 0:
                c, s = turn(t)
                r, i = r * c - i * s, r * s + i * c
            columns.append(jnp.concatenate([r, i], 0))
        res = dot3(span_w, split(jnp.concatenate(columns, 1)))
        for t in range(4):
            grid[pair, t] = res[:, t * LANES : (t + 1) * LANES]

    back_w = span[...]
    back_w = split(jnp.concatenate([back_w[:, :quarter], back_w[:, quarter:]], 0))
    lo = lax.broadcasted_iota(jnp.int32, (quarter, LANES), 1) < lines

    def q_copy(batch, dest, source):
        slots = pl.ds(*back_batches[batch])
        return pltpu.make_async_remote_copy(
            src_ref=q_send.at[dest, slots],
            dst_ref=q_recv.at[source, slots],
            send_sem=q_send_sem.at[batch, dest],
            recv_sem=q_recv_sem.at[batch, source],
            device_id={"pa": dest},
        )

    def q_start(batch):
        @pl.loop(1, groups)
        def _(k):
            dest = lax.rem(me + k, groups)

            @pl.when(dest < kept)
            def _():
                q_copy(batch, dest, me).start()

        first_slot, count = back_batches[batch]
        for slot in range(first_slot, first_slot + count):
            q_recv[me, slot] = q_send[me, slot]

    def q_wait(batch):
        @pl.loop(1, groups)
        def _(k):
            source = lax.rem(me + groups - k, groups)
            q_copy(batch, source, source).wait_recv()

    def y_back(columns, comps):
        res = dot3(back_w, split(jnp.concatenate(columns, 1)))
        sums = []
        for t in range(4):
            r = res[:quarter, t * LANES : (t + 1) * LANES]
            i = res[quarter:, t * LANES : (t + 1) * LANES]
            if t > 0:
                c, s = turn(t)
                r, i = r * c + i * s, i * c - r * s
            sums.append((r, i))
        (r0, i0), (r1, i1), (r2, i2), (r3, i3) = sums
        low = (r0 + r1 + r2 + r3, i0 + i1 + i2 + i3)
        high = (r0 - r2 + (i1 - i3), i0 - i2 - (r1 - r3))
        for base, (r, i), count in (
            (0, low, quarter // kyl),
            (quarter // kyl, high, kept - quarter // kyl),
        ):
            rolled_i, rolled_r = swap(i), swap(r)
            packed = [jnp.where(lo, r, rolled_i), jnp.where(lo, rolled_r, i)]
            for comp, value in zip(comps, packed):
                q_send[base : base + count, comp] = value[: count * kyl].reshape(count, kyl, LANES)

    pass_on()
    wait_batch(0)
    v_copy = pair_copy(3, recv.at[:, 0], g_other)
    v_copy.start()
    y_forward(0, field(1), field(0))
    wait_batch(1)
    v_copy.wait_recv()
    swirl_x = ky_all * swap(field(2)) - dz * g_other[...].reshape(half, LANES)
    y_forward(1, field(3), swirl_x)
    columns = []
    for t in range(4):
        product = grid[0, t] * grid[1, t]
        columns.append(product - swap(product))
    y_back(columns, (0,))
    q_start(0)
    wait_batch(2)
    y_forward(2, field(2), field(4))
    columns = []
    for t in range(4):
        speed, swirls, mixed = grid[0, t], grid[1, t], grid[2, t]
        x_part = swap(speed * mixed) - mixed * swirls
        y_part = mixed * swap(swirls) - speed * swap(mixed)
        columns.append(jnp.where(lo, x_part, swap(y_part)))
    y_back(columns, (1, 2))
    q_start(1)

    loads["to_wave"].wait()
    loads["mask"].wait()
    wave_w = split(to_wave[...])

    def x_back(slot, comp):
        rows = [
            jnp.concatenate([q_recv[2 * c, slot], q_recv[2 * c + 1, slot]], 1)
            for c in range(radix)
        ]
        res = dot3(split(jnp.concatenate(rows, 0)), wave_w)
        z = []
        for c in range(radix):
            r = res[c * kyl : (c + 1) * kyl, :LANES]
            i = res[c * kyl : (c + 1) * kyl, LANES:]
            if c > 0:
                tc = jnp.broadcast_to(line_turn[c : c + 1, :], (kyl, LANES))
                ts = jnp.broadcast_to(line_turn[radix + c : radix + c + 1, :], (kyl, LANES))
                r, i = r * tc + i * ts, i * tc - r * ts
            z.append((r, i))
        for a, values in enumerate(short_fft(z, -1.0)):
            at = slice(a * LANES, (a + 1) * LANES)
            gain = time_step * mask[:, at].astype(jnp.float32)
            for part in range(2):
                out[comp, 0, part, :, at] = out[comp, 0, part, :, at] + gain * values[part]

    @pl.when(me < kept)
    def _():
        q_wait(0)
        x_back(0, 2)

    w_copy = pair_copy(4, out.at[2, 0], w_other)
    w_copy.start()

    @pl.when(me < kept)
    def _():
        q_wait(1)
        x_back(1, 0)
        x_back(2, 1)

    kx_all = kx_ref[...]
    w_copy.wait_recv()
    for part, sign in ((0, -1.0), (1, 1.0)):
        u_next = out[0, 0, 1 - part]
        v_next = out[1, 0, 1 - part]
        div[0, part] = dz * w_other[part] + sign * (kx_all * u_next + ky_wide * v_next)

    for copy in vel_copies + [v_copy, w_copy]:
        copy.wait_send()

    @pl.when(middle)
    def _():
        for index in range(half_depth):
            hop_copy(index).wait_send()
            each_pass(index, lambda copy: copy.wait_send())

    for batch in range(len(field_batches)):

        @pl.loop(1, groups)
        def _(k):
            dest = lax.rem(me + k, groups)

            @pl.when(direct(dest) | (batch > 0))
            def _():
                batch_copy(batch, dest, me).wait_send()

    for batch in range(len(back_batches)):

        @pl.loop(1, groups)
        def _(k):
            dest = lax.rem(me + k, groups)

            @pl.when(dest < kept)
            def _():
                q_copy(batch, dest, me).wait_send()


def store_kernel(next_ref, div_ref, next_out, div_out, sem):
    copies = [pltpu.make_async_copy(next_ref.at[f], next_out.at[f], sem.at[f]) for f in range(3)]
    copies.append(pltpu.make_async_copy(div_ref, div_out, sem.at[3]))
    for copy in copies:
        copy.start()
    for copy in copies:
        copy.wait()


def in_one_kernel(velocity, mode_mask):
    groups = lax.axis_size("pa")
    kyl = velocity.shape[3]
    ncols = velocity.shape[4]
    lines = ncols // groups
    half = kyl * groups
    nrows = 2 * half
    kept = -(-(nrows // 3) // kyl)
    signed = np.where(np.arange(ncols) < ncols // 2, np.arange(ncols), np.arange(ncols) - ncols)
    kx = (np.float32(2.0 * math.pi / ncols) * signed.astype(np.float32))[None, :]
    operands = [velocity, mode_mask] + [jnp.asarray(t) for t in tables(ncols, nrows, lines)]
    operands.append(jnp.asarray(kx))
    f32 = jnp.float32
    halves = groups // PLANE // 2
    hbm = pl.BlockSpec(memory_space=pltpu.HBM)
    whole = pl.BlockSpec(memory_space=pl.ANY)
    vmem = pl.BlockSpec(memory_space=pltpu.VMEM)
    dma = pltpu.SemaphoreType.DMA
    shapes = (
        jax.ShapeDtypeStruct(velocity.shape, f32),
        jax.ShapeDtypeStruct(velocity.shape[1:], f32),
    )
    following, divergence = pl.pallas_call(
        functools.partial(kernel, groups, kept),
        out_shape=shapes,
        in_specs=[hbm] * len(operands),
        out_specs=(vmem, vmem),
        scratch_shapes=[pltpu.VMEM(t.shape, t.dtype) for t in operands]
        + [
            pltpu.VMEM((groups, 5, kyl, LANES), f32),
            pltpu.VMEM((groups, 5, kyl, LANES), f32),
            pltpu.VMEM((3, 2, kyl, ncols), f32),
            pltpu.VMEM((groups, kyl, LANES), f32),
            pltpu.VMEM((groups, 3, kyl, LANES), f32),
            pltpu.VMEM((groups, 3, kyl, LANES), f32),
            pltpu.VMEM((2, kyl, ncols), f32),
            pltpu.VMEM((3, 4, half // 2, LANES), f32),
            dma((10,)),
            dma((len(field_batches), groups)),
            dma((len(field_batches), groups)),
            dma((len(back_batches), groups)),
            dma((len(back_batches), groups)),
            dma((5,)),
            dma((5,)),
            pltpu.SemaphoreType.REGULAR((groups,)),
            pltpu.VMEM((halves, PLANE, field_batches[0][1], kyl, LANES), f32),
            dma((halves,)),
            dma((halves,)),
            dma((halves, PLANE)),
        ],
        compiler_params=pltpu.CompilerParams(collective_id=0, has_side_effects=True, vmem_limit_bytes=32 * 2**20),
    )(*[pltpu.with_memory_space_constraint(x, pltpu.HBM) for x in operands])
    return pl.pallas_call(
        store_kernel,
        out_shape=shapes,
        in_specs=[whole, whole],
        out_specs=(hbm, hbm),
        scratch_shapes=[dma((4,))],
        compiler_params=pltpu.CompilerParams(vmem_limit_bytes=2**20),
    )(following, divergence)


def on_device(velocity, mode_mask):
    groups = lax.axis_size("pa")
    kyl = velocity.shape[3]
    ncols = velocity.shape[4]
    fits = (
        lax.axis_size("gz") == 2
        and velocity.shape[1] == 1
        and kyl % 8 == 0
        and groups % (2 * PLANE) == 0
        and 2 * (ncols // groups) == LANES
        and (kyl * groups // 2) % LANES == 0
        and ncols % LANES == 0
        and nrows_cover(kyl * groups)
    )
    return in_one_kernel(velocity, mode_mask) if fits else by_steps(velocity, mode_mask)


def nrows_cover(half):
    return 2 * half // 3 > half // 2


def solution(mesh):
    placed = (P(None, "gz", None, "pa", None), P("pa", None))
    return jax.shard_map(
        on_device,
        mesh=mesh,
        in_specs=placed,
        out_specs=(P(None, "gz", None, "pa", None), P("gz", None, "pa", None)),
        check_vma=False,
    )
```

```python
import functools
import math

import jax
import jax.numpy as jnp
import numpy as np
from jax import lax
from jax.experimental import pallas as pl
from jax.experimental.pallas import tpu as pltpu
from jax.sharding import PartitionSpec as P

precise = lax.Precision.HIGHEST
time_step = 0.2
viscosity = 0.25


def extended(block, sides, width):
    for axis, dim in sides:
        count = lax.axis_size(axis)
        forward = [(i, i + 1) for i in range(count - 1)]
        backward = [(target, source) for source, target in forward]
        low = lax.ppermute(
            lax.slice_in_dim(block, block.shape[dim] - width, None, axis=dim), axis, forward
        )
        high = lax.ppermute(lax.slice_in_dim(block, 0, width, axis=dim), axis, backward)
        block = jnp.concatenate([low, block, high], axis=dim)
    return block


def phase_pair(rows, cols, period, sign):
    angle = 2.0 * math.pi / period * (rows[:, None] * cols[None, :] % period).astype(jnp.float32)
    return (jnp.cos(angle), sign * jnp.sin(angle))


def factor_sizes(length):
    second = 2 ** ((length.bit_length() - 1) // 2)
    return (length // second, second)


def factored(real, imag, sign, first, second, keep):
    used = real.shape[-1] // second
    lead = real.shape[:-1]
    a_index = jnp.arange(used, dtype=jnp.int32)
    c_index = jnp.arange(first, dtype=jnp.int32)
    b_index = jnp.arange(second, dtype=jnp.int32)
    d_index = jnp.arange(keep, dtype=jnp.int32)
    one_cos, one_sin = phase_pair(a_index, c_index, first, sign)
    turn_cos, turn_sin = phase_pair(c_index, b_index, first * second, sign)
    two_cos, two_sin = phase_pair(b_index, d_index, second, sign)
    x_real = real.reshape(lead + (used, second))
    a_real = jnp.einsum("...ab,ac->...cb", x_real, one_cos, precision=precise)
    a_imag = jnp.einsum("...ab,ac->...cb", x_real, one_sin, precision=precise)
    if imag is not None:
        x_imag = imag.reshape(lead + (used, second))
        a_real = a_real - jnp.einsum("...ab,ac->...cb", x_imag, one_sin, precision=precise)
        a_imag = a_imag + jnp.einsum("...ab,ac->...cb", x_imag, one_cos, precision=precise)
    t_real = a_real * turn_cos - a_imag * turn_sin
    t_imag = a_real * turn_sin + a_imag * turn_cos
    o_real = jnp.einsum("...cb,bd->...dc", t_real, two_cos, precision=precise) - jnp.einsum(
        "...cb,bd->...dc", t_imag, two_sin, precision=precise
    )
    o_imag = jnp.einsum("...cb,bd->...dc", t_real, two_sin, precision=precise) + jnp.einsum(
        "...cb,bd->...dc", t_imag, two_cos, precision=precise
    )
    return (o_real.reshape(lead + (keep * first,)), o_imag.reshape(lead + (keep * first,)))


def wall_first(padded):
    return 0.5 * (padded[2:] - padded[:-2])


def times_wave(wave, field):
    return jnp.stack([-wave * field[:, 1], wave * field[:, 0]], 1)


def by_steps(velocity, mode_mask):
    groups = lax.axis_size("pa")
    rank = lax.axis_index("pa")
    depth = velocity.shape[1]
    kyl = velocity.shape[3]
    ncols = velocity.shape[4]
    lines = ncols // groups
    half = kyl * groups
    nrows = 2 * half
    x_first, x_second = factor_sizes(ncols)
    y_first, y_second = factor_sizes(nrows)
    x_scale = 1.0 / math.sqrt(ncols)
    y_scale = 1.0 / math.sqrt(nrows)
    modes = jnp.arange(ncols, dtype=jnp.int32)
    signed = jnp.where(modes < ncols // 2, modes, modes - ncols)
    kx_wave = 2.0 * math.pi / ncols * signed.astype(jnp.float32)
    own_modes = rank * kyl + jnp.arange(kyl, dtype=jnp.int32)
    ky_wave = (2.0 * math.pi / nrows * own_modes.astype(jnp.float32))[:, None]
    span_index = jnp.arange(half, dtype=jnp.int32)
    weight = jnp.where(span_index == 0, 1.0, 2.0).astype(jnp.float32)

    def to_modes(received):
        count = received.shape[0]
        planes = received.shape[1]
        blocks = received.reshape(count, planes, 2, groups, lines, kyl)
        blocks = jnp.transpose(blocks, (0, 1, 2, 5, 3, 4)).reshape(count, planes, 2, kyl, ncols)
        h_real, h_imag = factored(
            blocks[:, :, 0], blocks[:, :, 1], -1.0, x_first, x_second, x_second
        )
        return jnp.stack([h_real, h_imag], 2) * x_scale

    padded = extended(velocity, (("gz", 1),), 1)
    u_spec = velocity[0]
    v_spec = velocity[1]
    w_spec = velocity[2]
    omega_x = times_wave(ky_wave, w_spec) - wall_first(padded[1])
    omega_y = wall_first(padded[0]) - times_wave(kx_wave, w_spec)
    omega_z = times_wave(kx_wave, v_spec) - times_wave(ky_wave, u_spec)
    vorticity = jnp.stack([omega_x, omega_y, omega_z], 0)
    both = jnp.concatenate([velocity, vorticity], 0)
    count = both.shape[0]
    g_real, g_imag = factored(both[:, :, 0], both[:, :, 1], 1.0, x_first, x_second, x_second)
    joined = jnp.stack([g_real, g_imag], 2) * x_scale
    joined = jnp.swapaxes(joined, 3, 4)
    received = lax.all_to_all(
        joined.reshape(count, depth, 2, groups, lines * kyl),
        "pa",
        split_axis=3,
        concat_axis=3,
        tiled=True,
    )
    to_count = received.shape[0]
    planes = received.shape[1]
    blocks = received.reshape(to_count, planes, 2, groups, lines, kyl)
    blocks = jnp.transpose(blocks, (0, 1, 2, 4, 3, 5)).reshape(to_count, planes, 2, lines, half)
    blocks = blocks * weight
    p_real, p_imag = factored(blocks[:, :, 0], blocks[:, :, 1], 1.0, y_first, y_second, y_second)
    grid = p_real * y_scale
    speed_grid = grid[:3]
    swirl_grid = grid[3:]
    u_grid = speed_grid[0]
    v_grid = speed_grid[1]
    w_grid = speed_grid[2]
    cross = jnp.stack(
        [
            v_grid * swirl_grid[2] - w_grid * swirl_grid[1],
            w_grid * swirl_grid[0] - u_grid * swirl_grid[2],
            u_grid * swirl_grid[1] - v_grid * swirl_grid[0],
        ],
        0,
    )
    count = cross.shape[0]
    q_real, q_imag = factored(cross, None, -1.0, y_first, y_second, y_second // 2)
    joined = jnp.stack([q_real, q_imag], 2) * y_scale
    joined = joined.reshape(count, depth, 2, lines, groups, kyl)
    joined = jnp.transpose(joined, (0, 1, 2, 4, 3, 5))
    nonlinear = to_modes(
        lax.all_to_all(
            joined.reshape(count, depth, 2, groups, lines * kyl),
            "pa",
            split_axis=3,
            concat_axis=3,
            tiled=True,
        )
    )
    mask = mode_mask.astype(jnp.float32)
    viscous = padded[:, 2:] - 2.0 * padded[:, 1:-1] + padded[:, :-2]
    viscous = viscous - (kx_wave * kx_wave + ky_wave * ky_wave) * velocity
    following = velocity + time_step * (nonlinear * mask + viscosity * viscous)
    w_padded = extended(following[2], (("gz", 0),), 1)
    divergence = (
        times_wave(kx_wave, following[0]) + times_wave(ky_wave, following[1]) + wall_first(w_padded)
    )
    return (following, divergence)


LANES = 128


def split(value):
    high = value.astype(jnp.bfloat16)
    low = (value - high.astype(jnp.float32)).astype(jnp.bfloat16)
    return high, low


def dot3(left, right):
    def dot(a, b):
        return jnp.dot(a, b, preferred_element_type=jnp.float32)

    return dot(left[0], right[0]) + (dot(left[0], right[1]) + dot(left[1], right[0]))


def turned(z, k, n, sign):
    real, imag = z
    if k == 0:
        return z
    if 4 * k == n:
        return (-imag, real) if sign > 0 else (imag, -real)
    c = math.cos(2.0 * math.pi * k / n)
    s = sign * math.sin(2.0 * math.pi * k / n)
    return (real * c - imag * s, real * s + imag * c)


def short_fft(z, sign):
    n = len(z)
    if n == 1:
        return z
    even = short_fft(z[0::2], sign)
    odd = short_fft(z[1::2], sign)
    low, high = [], []
    for k in range(n // 2):
        t = turned(odd[k], k, n, sign)
        low.append((even[k][0] + t[0], even[k][1] + t[1]))
        high.append((even[k][0] - t[0], even[k][1] - t[1]))
    return low + high


@functools.lru_cache(None)
def tables(ncols, nrows, lines):
    radix = ncols // LANES
    quarter = nrows // 4
    b = np.arange(LANES)
    angle = 2.0 * np.pi * (np.outer(b, b) % LANES) / LANES
    c, s = np.cos(angle), np.sin(angle)
    order = np.concatenate(
        [p * LANES + h * lines + np.arange(lines) for h in range(LANES // lines) for p in (0, 1)]
    )
    to_grid = np.block([[c, s], [-s, c]])[:, order] / math.sqrt(ncols)
    to_wave = np.block([[c, -s], [s, c]])[order, :] / math.sqrt(ncols) / 2.0
    q = np.arange(quarter)
    angle = 2.0 * np.pi * (np.outer(q, q) % quarter) / quarter
    span = np.concatenate([np.cos(angle), -np.sin(angle)], 1) * (2.0 / math.sqrt(nrows))
    angle = 2.0 * np.pi * np.outer(q, np.arange(4)) / nrows
    span_turn = np.concatenate([np.cos(angle), np.sin(angle)], 1)
    angle = 2.0 * np.pi * np.outer(np.arange(radix), b) / ncols
    line_turn = np.concatenate([np.cos(angle), np.sin(angle)], 0)
    return [np.asarray(t, np.float32) for t in (to_grid, to_wave, span, span_turn, line_turn)]


PLANE = 4
NEAR = 1
field_batches = ((0, 2), (2, 2), (4, 1))
back_batches = ((0, 1), (1, 2))


def kernel(
    groups, kept,
    vel_hbm, mask_hbm, to_grid_hbm, to_wave_hbm, span_hbm, span_turn_hbm, line_turn_hbm, kx_hbm,
    out, div,
    vel, mask, to_grid, to_wave, span, span_turn, line_turn, kx_ref,
    send, recv, vel_other, g_other, q_send, q_recv, w_other, grid,
    load_sem, send_sem, recv_sem, q_send_sem, q_recv_sem, pair_sem, pair_recv_sem, ready,
    hop, hop_sem, hop_recv_sem, pass_sem,
):
    me = lax.axis_index("pa")
    side = lax.axis_index("gz")
    partner = {"gz": 1 - side}
    kyl = vel.shape[3]
    ncols = vel.shape[4]
    lines = ncols // groups
    half = kyl * groups
    nrows = 2 * half
    quarter = half // 2
    radix = ncols // LANES
    dz = jnp.where(side == 0, 0.5, -0.5).astype(jnp.float32)

    depth = groups // PLANE
    diameter = depth + 1
    layer = me // PLANE
    column = lax.rem(me, PLANE)
    flipped = [column]
    for step in (1, 2):
        flipped += [f + step - 2 * step * lax.rem(f // step, 2) for f in flipped]
    reach = sorted(range(1 - depth, depth), key=lambda d: (-abs(d), -d))

    def columns_within(shift, low, high):
        return [c for c in range(PLANE) if low <= abs(shift) + c.bit_count() <= high]

    def each_peer(low, high, act):
        for shift in reach:
            chosen = columns_within(shift, low, high)
            if not chosen:
                continue

            def visit(shift=shift, chosen=chosen):
                for c in chosen:
                    act((layer + shift) * PLANE + flipped[c])

            if shift == 0:
                visit()
            else:
                pl.when((layer + shift >= 0) & (layer + shift < depth))(visit)

    def peers(low, high):
        total = 0
        for shift in reach:
            count = len(columns_within(shift, low, high))
            inside = (layer + shift >= 0) & (layer + shift < depth)
            total = total + jnp.where(inside, count, 0)
        return total

    barrier = pltpu.get_barrier_semaphore()
    each_peer(1, NEAR, lambda d: pl.semaphore_signal(barrier, inc=1, device_id={"pa": d}))
    pl.semaphore_signal(barrier, inc=1, device_id=partner)

    loads = {}
    for index, (name, src, dst) in enumerate(
        (
            ("v", vel_hbm.at[1], vel.at[1]),
            ("to_grid", to_grid_hbm, to_grid),
            ("line_turn", line_turn_hbm, line_turn),
            ("u", vel_hbm.at[0], vel.at[0]),
            ("w", vel_hbm.at[2], vel.at[2]),
            ("kx", kx_hbm, kx_ref),
            ("span", span_hbm, span),
            ("span_turn", span_turn_hbm, span_turn),
            ("to_wave", to_wave_hbm, to_wave),
            ("mask", mask_hbm, mask),
        )
    ):
        loads[name] = pltpu.make_async_copy(src, dst, load_sem.at[index])
        loads[name].start()

    own_n = me * kyl + lax.broadcasted_iota(jnp.int32, (kyl, LANES), 0)
    ky_own = 2.0 * math.pi / nrows * own_n.astype(jnp.float32)
    weight = jnp.where(own_n == 0, 0.5, 1.0).astype(jnp.float32)
    loads["v"].wait()
    loads["to_grid"].wait()
    loads["line_turn"].wait()
    grid_w = split(to_grid[...])

    def block(ref, a):
        return ref[:, a * LANES : (a + 1) * LANES]

    def kx_at(a):
        return jnp.broadcast_to(kx_ref[:, a * LANES : (a + 1) * LANES], (kyl, LANES))

    def spec(comp, a):
        at = slice(a * LANES, (a + 1) * LANES)
        return (vel[comp, 0, 0, :, at], vel[comp, 0, 1, :, at])

    def x_forward(slot, z):
        z = [(r * weight, i * weight) for r, i in z]
        lhs = []
        for c, (r, i) in enumerate(short_fft(z, 1.0)):
            if c > 0:
                tc = jnp.broadcast_to(line_turn[c : c + 1, :], (kyl, LANES))
                ts = jnp.broadcast_to(line_turn[radix + c : radix + c + 1, :], (kyl, LANES))
                r, i = r * tc - i * ts, r * ts + i * tc
            lhs.append(jnp.concatenate([r, i], 1))
        res = dot3(split(jnp.concatenate(lhs, 0)), grid_w)
        for c in range(radix):
            rows = res[c * kyl : (c + 1) * kyl]
            send[2 * c, slot] = rows[:, :LANES]
            send[2 * c + 1, slot] = rows[:, LANES:]

    def batch_copy(batch, dest, source):
        slots = pl.ds(*field_batches[batch])
        return pltpu.make_async_remote_copy(
            src_ref=send.at[dest, slots],
            dst_ref=recv.at[source, slots],
            send_sem=send_sem.at[batch, dest],
            recv_sem=recv_sem.at[batch, source],
            device_id={"pa": dest},
        )

    def send_batch(batch):
        @pl.loop(1, groups)
        def _(k):
            batch_copy(batch, lax.rem(me + k, groups), me).start()

        keep_own(batch)

    def keep_own(batch):
        first_slot, count = field_batches[batch]
        for slot in range(first_slot, first_slot + count):
            recv[me, slot] = send[me, slot]

    def wait_batch(batch):
        @pl.loop(1, groups)
        def _(k):
            source = lax.rem(me + groups - k, groups)

            @pl.when((source != mate) | jnp.logical_not(middle) | (batch > 0))
            def _():
                batch_copy(batch, source, source).wait_recv()

    def pair_copy(index, src, dst):
        return pltpu.make_async_remote_copy(
            src_ref=src,
            dst_ref=dst,
            send_sem=pair_sem.at[index],
            recv_sem=pair_recv_sem.at[index],
            device_id=partner,
        )

    x_forward(0, [spec(1, a) for a in range(radix)])
    pl.semaphore_wait(barrier, peers(1, NEAR) + 1)

    half_depth = depth // 2
    upper = layer >= half_depth
    middle = (layer == half_depth) | (layer == half_depth - 1)
    mate = jnp.where(upper, me - PLANE, me + PLANE)
    own_half = jnp.where(upper, groups // 2, 0)
    other_half = groups // 2 - own_half
    lead = pl.ds(*field_batches[0])

    def hop_copy(index, slot):
        return pltpu.make_async_remote_copy(
            src_ref=send.at[pl.ds(other_half + index * PLANE, PLANE), slot],
            dst_ref=hop.at[index, :, slot],
            send_sem=hop_sem.at[index, slot],
            recv_sem=hop_recv_sem.at[index, slot],
            device_id={"pa": mate},
        )

    def send_hops(slot):
        @pl.when(middle)
        def _():
            for index in range(half_depth):
                hop_copy(index, slot).start()

    def pass_copy(index, c):
        return pltpu.make_async_remote_copy(
            src_ref=hop.at[index, c],
            dst_ref=recv.at[mate, lead],
            send_sem=pass_sem.at[index, c],
            recv_sem=recv_sem.at[0, mate],
            device_id={"pa": own_half + index * PLANE + c},
        )

    def each_pass(index, act):
        for c in range(PLANE):

            @pl.when(own_half + index * PLANE + c != me)
            def _():
                act(pass_copy(index, c))

    def pass_on():
        @pl.when(middle)
        def _():
            for index in range(half_depth):
                for slot in range(field_batches[0][1]):
                    hop_copy(index, slot).wait_recv()
                each_pass(index, lambda copy: copy.start())
                for c in range(PLANE):

                    @pl.when(own_half + index * PLANE + c == me)
                    def _():
                        recv[mate, lead] = hop[index, c]

    def direct(dest):
        return jnp.logical_not(middle & ((dest >= groups // 2) != upper))

    steps = []
    known = NEAR
    while known < diameter:
        steps.append(min(known, diameter - known))
        known += steps[-1]

    def tell(index):
        if index < len(steps):
            each_peer(
                1,
                steps[index],
                lambda d: pl.semaphore_signal(ready.at[index], inc=1, device_id={"pa": d}),
            )

    def hear(index):
        if index < len(steps):
            pl.semaphore_wait(ready.at[index], peers(1, steps[index]))
            tell(index + 1)

    tell(0)

    send_hops(0)
    loads["u"].wait()
    x_forward(1, [spec(0, a) for a in range(radix)])
    send_hops(1)
    loads["w"].wait()
    loads["kx"].wait()
    keep_own(0)
    vel_copies = [pair_copy(f, vel.at[f, 0], vel_other.at[f]) for f in range(3)]
    for copy in vel_copies:
        copy.start()
    x_forward(2, [spec(2, a) for a in range(radix)])
    hear(0)
    vel_copies[0].wait_recv()
    swirl = []
    for a in range(radix):
        w, kx = spec(2, a), kx_at(a)
        at = slice(a * LANES, (a + 1) * LANES)
        swirl.append((dz * vel_other[0, 0, :, at] + kx * w[1], dz * vel_other[0, 1, :, at] - kx * w[0]))
    x_forward(3, swirl)
    for index in range(1, len(steps)):
        hear(index)

    @pl.loop(1, groups)
    def _(k):
        dest = lax.rem(me + k, groups)

        @pl.when(direct(dest))
        def _():
            batch_copy(0, dest, me).start()

    send_batch(1)
    swirl = []
    for a in range(radix):
        v, u, kx = spec(1, a), spec(0, a), kx_at(a)
        swirl.append((ky_own * u[1] - kx * v[1], kx * v[0] - ky_own * u[0]))
    x_forward(4, swirl)
    send_batch(2)

    vel_copies[1].wait_recv()
    vel_copies[2].wait_recv()
    ky_wide = ky_own[:, :1]
    square = kx_ref[...] * kx_ref[...] + ky_wide * ky_wide
    for f in range(3):
        for part in range(2):
            own = vel[f, 0, part]
            viscous = vel_other[f, part] - 2.0 * own - square * own
            out[f, 0, part] = own + time_step * viscosity * viscous

    loads["span"].wait()
    loads["span_turn"].wait()
    span_w = split(span[...])
    lane = lax.broadcasted_iota(jnp.int32, (half, LANES), 1)
    first = lane < lines
    all_n = lax.broadcasted_iota(jnp.int32, (half, LANES), 0)
    ky_all = 2.0 * math.pi / nrows * all_n.astype(jnp.float32)
    ky_all = jnp.where(first, -ky_all, ky_all)

    def swap(value):
        return pltpu.roll(value, lines, 1)

    def turn(t):
        c = jnp.broadcast_to(span_turn[:, t : t + 1], (quarter, LANES))
        s = jnp.broadcast_to(span_turn[:, 4 + t : 5 + t], (quarter, LANES))
        return c, s

    def field(slot):
        return recv[:, slot].reshape(half, LANES)

    def y_forward(pair, one, two):
        real = jnp.where(first, one, swap(two))
        imag = jnp.where(first, swap(one), two)
        rl, rh, il, ih = real[:quarter], real[quarter:], imag[:quarter], imag[quarter:]
        columns = []
        for t, (r, i) in enumerate(
            [(rl + rh, il + ih), (rl - ih, il + rh), (rl - rh, il - ih), (rl + ih, il - rh)]
        ):
            if t > 0:
                c, s = turn(t)
                r, i = r * c - i * s, r * s + i * c
            columns.append(jnp.concatenate([r, i], 0))
        res = dot3(span_w, split(jnp.concatenate(columns, 1)))
        for t in range(4):
            grid[pair, t] = res[:, t * LANES : (t + 1) * LANES]

    back_w = span[...]
    back_w = split(jnp.concatenate([back_w[:, :quarter], back_w[:, quarter:]], 0))
    lo = lax.broadcasted_iota(jnp.int32, (quarter, LANES), 1) < lines

    def q_copy(batch, dest, source):
        slots = pl.ds(*back_batches[batch])
        return pltpu.make_async_remote_copy(
            src_ref=q_send.at[dest, slots],
            dst_ref=q_recv.at[source, slots],
            send_sem=q_send_sem.at[batch, dest],
            recv_sem=q_recv_sem.at[batch, source],
            device_id={"pa": dest},
        )

    def q_start(batch):
        @pl.loop(1, groups)
        def _(k):
            dest = lax.rem(me + k, groups)

            @pl.when(dest < kept)
            def _():
                q_copy(batch, dest, me).start()

        first_slot, count = back_batches[batch]
        for slot in range(first_slot, first_slot + count):
            q_recv[me, slot] = q_send[me, slot]

    def q_wait(batch, first_source, last_source):
        @pl.loop(first_source, last_source)
        def _(source):
            @pl.when(source != me)
            def _():
                q_copy(batch, source, source).wait_recv()

    def y_back(columns, comps):
        res = dot3(back_w, split(jnp.concatenate(columns, 1)))
        sums = []
        for t in range(4):
            r = res[:quarter, t * LANES : (t + 1) * LANES]
            i = res[quarter:, t * LANES : (t + 1) * LANES]
            if t > 0:
                c, s = turn(t)
                r, i = r * c + i * s, i * c - r * s
            sums.append((r, i))
        (r0, i0), (r1, i1), (r2, i2), (r3, i3) = sums
        low = (r0 + r1 + r2 + r3, i0 + i1 + i2 + i3)
        high = (r0 - r2 + (i1 - i3), i0 - i2 - (r1 - r3))
        for base, (r, i), count in (
            (0, low, quarter // kyl),
            (quarter // kyl, high, kept - quarter // kyl),
        ):
            rolled_i, rolled_r = swap(i), swap(r)
            packed = [jnp.where(lo, r, rolled_i), jnp.where(lo, rolled_r, i)]
            for comp, value in zip(comps, packed):
                q_send[base : base + count, comp] = value[: count * kyl].reshape(count, kyl, LANES)

    pass_on()
    wait_batch(0)
    v_copy = pair_copy(3, recv.at[:, 0], g_other)
    v_copy.start()
    y_forward(0, field(1), field(0))
    wait_batch(1)
    v_copy.wait_recv()
    swirl_x = ky_all * swap(field(2)) - dz * g_other[...].reshape(half, LANES)
    y_forward(1, field(3), swirl_x)
    columns = []
    for t in range(4):
        product = grid[0, t] * grid[1, t]
        columns.append(product - swap(product))
    y_back(columns, (0,))
    q_start(0)
    wait_batch(2)
    y_forward(2, field(2), field(4))
    columns = []
    for t in range(4):
        speed, swirls, mixed = grid[0, t], grid[1, t], grid[2, t]
        x_part = swap(speed * mixed) - mixed * swirls
        y_part = mixed * swap(swirls) - speed * swap(mixed)
        columns.append(jnp.where(lo, x_part, swap(y_part)))
    y_back(columns, (1, 2))
    q_start(1)

    loads["to_wave"].wait()
    loads["mask"].wait()
    wave_w = split(to_wave[...])

    def x_lines(slot, residues):
        rows = [
            jnp.concatenate([q_recv[2 * c, slot], q_recv[2 * c + 1, slot]], 1) for c in residues
        ]
        res = dot3(split(jnp.concatenate(rows, 0)), wave_w)
        return [res[j * kyl : (j + 1) * kyl] for j in range(len(residues))]

    def x_back(comp, lines_of):
        z = []
        for c in range(radix):
            r = lines_of[c][:, :LANES]
            i = lines_of[c][:, LANES:]
            if c > 0:
                tc = jnp.broadcast_to(line_turn[c : c + 1, :], (kyl, LANES))
                ts = jnp.broadcast_to(line_turn[radix + c : radix + c + 1, :], (kyl, LANES))
                r, i = r * tc + i * ts, i * tc - r * ts
            z.append((r, i))
        for a, values in enumerate(short_fft(z, -1.0)):
            at = slice(a * LANES, (a + 1) * LANES)
            gain = time_step * mask[:, at].astype(jnp.float32)
            for part in range(2):
                out[comp, 0, part, :, at] = out[comp, 0, part, :, at] + gain * values[part]

    @pl.when(me < kept)
    def _():
        q_wait(0, 0, groups)
        x_back(2, x_lines(0, range(radix)))

    w_copy = pair_copy(4, out.at[2, 0], w_other)
    w_copy.start()

    for copy in vel_copies + [v_copy]:
        copy.wait_send()

    @pl.when(middle)
    def _():
        for index in range(half_depth):
            for slot in range(field_batches[0][1]):
                hop_copy(index, slot).wait_send()
            each_pass(index, lambda copy: copy.wait_send())

    for batch in range(len(field_batches)):

        @pl.loop(1, groups)
        def _(k):
            dest = lax.rem(me + k, groups)

            @pl.when(direct(dest) | (batch > 0))
            def _():
                batch_copy(batch, dest, me).wait_send()

    for batch in range(len(back_batches)):

        @pl.loop(1, groups)
        def _(k):
            dest = lax.rem(me + k, groups)

            @pl.when(dest < kept)
            def _():
                q_copy(batch, dest, me).wait_send()

    @pl.when(me < kept)
    def _():
        half_radix = radix // 2
        q_wait(1, 0, groups // 2)
        near = [x_lines(slot, range(half_radix)) for slot in (1, 2)]
        q_wait(1, groups // 2, groups)
        for slot in (1, 2):
            x_back(slot - 1, near[slot - 1] + x_lines(slot, range(half_radix, radix)))

    kx_all = kx_ref[...]
    w_copy.wait_recv()
    for part, sign in ((0, -1.0), (1, 1.0)):
        u_next = out[0, 0, 1 - part]
        v_next = out[1, 0, 1 - part]
        div[0, part] = dz * w_other[part] + sign * (kx_all * u_next + ky_wide * v_next)

    w_copy.wait_send()


def store_kernel(next_ref, div_ref, next_out, div_out, sem):
    copies = [
        pltpu.make_async_copy(next_ref.at[f, 0, p], next_out.at[f, 0, p], sem.at[2 * f + p])
        for f in range(3)
        for p in range(2)
    ]
    copies += [
        pltpu.make_async_copy(div_ref.at[0, p], div_out.at[0, p], sem.at[6 + p]) for p in range(2)
    ]
    for copy in copies:
        copy.start()
    for copy in copies:
        copy.wait()


def in_one_kernel(velocity, mode_mask):
    groups = lax.axis_size("pa")
    kyl = velocity.shape[3]
    ncols = velocity.shape[4]
    lines = ncols // groups
    half = kyl * groups
    nrows = 2 * half
    kept = -(-(nrows // 3) // kyl)
    signed = np.where(np.arange(ncols) < ncols // 2, np.arange(ncols), np.arange(ncols) - ncols)
    kx = (np.float32(2.0 * math.pi / ncols) * signed.astype(np.float32))[None, :]
    operands = [velocity, mode_mask] + [jnp.asarray(t) for t in tables(ncols, nrows, lines)]
    operands.append(jnp.asarray(kx))
    f32 = jnp.float32
    halves = groups // PLANE // 2
    hbm = pl.BlockSpec(memory_space=pltpu.HBM)
    whole = pl.BlockSpec(memory_space=pl.ANY)
    vmem = pl.BlockSpec(memory_space=pltpu.VMEM)
    dma = pltpu.SemaphoreType.DMA
    shapes = (
        jax.ShapeDtypeStruct(velocity.shape, f32),
        jax.ShapeDtypeStruct(velocity.shape[1:], f32),
    )
    following, divergence = pl.pallas_call(
        functools.partial(kernel, groups, kept),
        out_shape=shapes,
        in_specs=[hbm] * len(operands),
        out_specs=(vmem, vmem),
        scratch_shapes=[pltpu.VMEM(t.shape, t.dtype) for t in operands]
        + [
            pltpu.VMEM((groups, 5, kyl, LANES), f32),
            pltpu.VMEM((groups, 5, kyl, LANES), f32),
            pltpu.VMEM((3, 2, kyl, ncols), f32),
            pltpu.VMEM((groups, kyl, LANES), f32),
            pltpu.VMEM((groups, 3, kyl, LANES), f32),
            pltpu.VMEM((groups, 3, kyl, LANES), f32),
            pltpu.VMEM((2, kyl, ncols), f32),
            pltpu.VMEM((3, 4, half // 2, LANES), f32),
            dma((10,)),
            dma((len(field_batches), groups)),
            dma((len(field_batches), groups)),
            dma((len(back_batches), groups)),
            dma((len(back_batches), groups)),
            dma((5,)),
            dma((5,)),
            pltpu.SemaphoreType.REGULAR((groups,)),
            pltpu.VMEM((halves, PLANE, field_batches[0][1], kyl, LANES), f32),
            dma((halves, field_batches[0][1])),
            dma((halves, field_batches[0][1])),
            dma((halves, PLANE)),
        ],
        compiler_params=pltpu.CompilerParams(collective_id=0, has_side_effects=True, vmem_limit_bytes=32 * 2**20),
    )(*[pltpu.with_memory_space_constraint(x, pltpu.HBM) for x in operands])
    return pl.pallas_call(
        store_kernel,
        out_shape=shapes,
        in_specs=[whole, whole],
        out_specs=(hbm, hbm),
        scratch_shapes=[dma((8,))],
        compiler_params=pltpu.CompilerParams(vmem_limit_bytes=2**20),
    )(following, divergence)


def on_device(velocity, mode_mask):
    groups = lax.axis_size("pa")
    kyl = velocity.shape[3]
    ncols = velocity.shape[4]
    fits = (
        lax.axis_size("gz") == 2
        and velocity.shape[1] == 1
        and kyl % 8 == 0
        and groups % (2 * PLANE) == 0
        and 2 * (ncols // groups) == LANES
        and (kyl * groups // 2) % LANES == 0
        and ncols % LANES == 0
        and nrows_cover(kyl * groups)
    )
    return in_one_kernel(velocity, mode_mask) if fits else by_steps(velocity, mode_mask)


def nrows_cover(half):
    return 2 * half // 3 > half // 2


def solution(mesh):
    placed = (P(None, "gz", None, "pa", None), P("pa", None))
    return jax.shard_map(
        on_device,
        mesh=mesh,
        in_specs=placed,
        out_specs=(P(None, "gz", None, "pa", None), P("gz", None, "pa", None)),
        check_vma=False,
    )
```

```python
import functools
import math

import jax
import jax.numpy as jnp
import numpy as np
from jax import lax
from jax.experimental import pallas as pl
from jax.experimental.pallas import tpu as pltpu
from jax.sharding import PartitionSpec as P

precise = lax.Precision.HIGHEST
time_step = 0.2
viscosity = 0.25


def extended(block, sides, width):
    for axis, dim in sides:
        count = lax.axis_size(axis)
        forward = [(i, i + 1) for i in range(count - 1)]
        backward = [(target, source) for source, target in forward]
        low = lax.ppermute(
            lax.slice_in_dim(block, block.shape[dim] - width, None, axis=dim), axis, forward
        )
        high = lax.ppermute(lax.slice_in_dim(block, 0, width, axis=dim), axis, backward)
        block = jnp.concatenate([low, block, high], axis=dim)
    return block


def phase_pair(rows, cols, period, sign):
    angle = 2.0 * math.pi / period * (rows[:, None] * cols[None, :] % period).astype(jnp.float32)
    return (jnp.cos(angle), sign * jnp.sin(angle))


def factor_sizes(length):
    second = 2 ** ((length.bit_length() - 1) // 2)
    return (length // second, second)


def factored(real, imag, sign, first, second, keep):
    used = real.shape[-1] // second
    lead = real.shape[:-1]
    a_index = jnp.arange(used, dtype=jnp.int32)
    c_index = jnp.arange(first, dtype=jnp.int32)
    b_index = jnp.arange(second, dtype=jnp.int32)
    d_index = jnp.arange(keep, dtype=jnp.int32)
    one_cos, one_sin = phase_pair(a_index, c_index, first, sign)
    turn_cos, turn_sin = phase_pair(c_index, b_index, first * second, sign)
    two_cos, two_sin = phase_pair(b_index, d_index, second, sign)
    x_real = real.reshape(lead + (used, second))
    a_real = jnp.einsum("...ab,ac->...cb", x_real, one_cos, precision=precise)
    a_imag = jnp.einsum("...ab,ac->...cb", x_real, one_sin, precision=precise)
    if imag is not None:
        x_imag = imag.reshape(lead + (used, second))
        a_real = a_real - jnp.einsum("...ab,ac->...cb", x_imag, one_sin, precision=precise)
        a_imag = a_imag + jnp.einsum("...ab,ac->...cb", x_imag, one_cos, precision=precise)
    t_real = a_real * turn_cos - a_imag * turn_sin
    t_imag = a_real * turn_sin + a_imag * turn_cos
    o_real = jnp.einsum("...cb,bd->...dc", t_real, two_cos, precision=precise) - jnp.einsum(
        "...cb,bd->...dc", t_imag, two_sin, precision=precise
    )
    o_imag = jnp.einsum("...cb,bd->...dc", t_real, two_sin, precision=precise) + jnp.einsum(
        "...cb,bd->...dc", t_imag, two_cos, precision=precise
    )
    return (o_real.reshape(lead + (keep * first,)), o_imag.reshape(lead + (keep * first,)))


def wall_first(padded):
    return 0.5 * (padded[2:] - padded[:-2])


def times_wave(wave, field):
    return jnp.stack([-wave * field[:, 1], wave * field[:, 0]], 1)


def by_steps(velocity, mode_mask):
    groups = lax.axis_size("pa")
    rank = lax.axis_index("pa")
    depth = velocity.shape[1]
    kyl = velocity.shape[3]
    ncols = velocity.shape[4]
    lines = ncols // groups
    half = kyl * groups
    nrows = 2 * half
    x_first, x_second = factor_sizes(ncols)
    y_first, y_second = factor_sizes(nrows)
    x_scale = 1.0 / math.sqrt(ncols)
    y_scale = 1.0 / math.sqrt(nrows)
    modes = jnp.arange(ncols, dtype=jnp.int32)
    signed = jnp.where(modes < ncols // 2, modes, modes - ncols)
    kx_wave = 2.0 * math.pi / ncols * signed.astype(jnp.float32)
    own_modes = rank * kyl + jnp.arange(kyl, dtype=jnp.int32)
    ky_wave = (2.0 * math.pi / nrows * own_modes.astype(jnp.float32))[:, None]
    span_index = jnp.arange(half, dtype=jnp.int32)
    weight = jnp.where(span_index == 0, 1.0, 2.0).astype(jnp.float32)

    def to_modes(received):
        count = received.shape[0]
        planes = received.shape[1]
        blocks = received.reshape(count, planes, 2, groups, lines, kyl)
        blocks = jnp.transpose(blocks, (0, 1, 2, 5, 3, 4)).reshape(count, planes, 2, kyl, ncols)
        h_real, h_imag = factored(
            blocks[:, :, 0], blocks[:, :, 1], -1.0, x_first, x_second, x_second
        )
        return jnp.stack([h_real, h_imag], 2) * x_scale

    padded = extended(velocity, (("gz", 1),), 1)
    u_spec = velocity[0]
    v_spec = velocity[1]
    w_spec = velocity[2]
    omega_x = times_wave(ky_wave, w_spec) - wall_first(padded[1])
    omega_y = wall_first(padded[0]) - times_wave(kx_wave, w_spec)
    omega_z = times_wave(kx_wave, v_spec) - times_wave(ky_wave, u_spec)
    vorticity = jnp.stack([omega_x, omega_y, omega_z], 0)
    both = jnp.concatenate([velocity, vorticity], 0)
    count = both.shape[0]
    g_real, g_imag = factored(both[:, :, 0], both[:, :, 1], 1.0, x_first, x_second, x_second)
    joined = jnp.stack([g_real, g_imag], 2) * x_scale
    joined = jnp.swapaxes(joined, 3, 4)
    received = lax.all_to_all(
        joined.reshape(count, depth, 2, groups, lines * kyl),
        "pa",
        split_axis=3,
        concat_axis=3,
        tiled=True,
    )
    to_count = received.shape[0]
    planes = received.shape[1]
    blocks = received.reshape(to_count, planes, 2, groups, lines, kyl)
    blocks = jnp.transpose(blocks, (0, 1, 2, 4, 3, 5)).reshape(to_count, planes, 2, lines, half)
    blocks = blocks * weight
    p_real, p_imag = factored(blocks[:, :, 0], blocks[:, :, 1], 1.0, y_first, y_second, y_second)
    grid = p_real * y_scale
    speed_grid = grid[:3]
    swirl_grid = grid[3:]
    u_grid = speed_grid[0]
    v_grid = speed_grid[1]
    w_grid = speed_grid[2]
    cross = jnp.stack(
        [
            v_grid * swirl_grid[2] - w_grid * swirl_grid[1],
            w_grid * swirl_grid[0] - u_grid * swirl_grid[2],
            u_grid * swirl_grid[1] - v_grid * swirl_grid[0],
        ],
        0,
    )
    count = cross.shape[0]
    q_real, q_imag = factored(cross, None, -1.0, y_first, y_second, y_second // 2)
    joined = jnp.stack([q_real, q_imag], 2) * y_scale
    joined = joined.reshape(count, depth, 2, lines, groups, kyl)
    joined = jnp.transpose(joined, (0, 1, 2, 4, 3, 5))
    nonlinear = to_modes(
        lax.all_to_all(
            joined.reshape(count, depth, 2, groups, lines * kyl),
            "pa",
            split_axis=3,
            concat_axis=3,
            tiled=True,
        )
    )
    mask = mode_mask.astype(jnp.float32)
    viscous = padded[:, 2:] - 2.0 * padded[:, 1:-1] + padded[:, :-2]
    viscous = viscous - (kx_wave * kx_wave + ky_wave * ky_wave) * velocity
    following = velocity + time_step * (nonlinear * mask + viscosity * viscous)
    w_padded = extended(following[2], (("gz", 0),), 1)
    divergence = (
        times_wave(kx_wave, following[0]) + times_wave(ky_wave, following[1]) + wall_first(w_padded)
    )
    return (following, divergence)


LANES = 128


def split(value):
    high = value.astype(jnp.bfloat16)
    low = (value - high.astype(jnp.float32)).astype(jnp.bfloat16)
    return high, low


def dot3(left, right):
    def dot(a, b):
        return jnp.dot(a, b, preferred_element_type=jnp.float32)

    return dot(left[0], right[0]) + (dot(left[0], right[1]) + dot(left[1], right[0]))


def turned(z, k, n, sign):
    real, imag = z
    if k == 0:
        return z
    if 4 * k == n:
        return (-imag, real) if sign > 0 else (imag, -real)
    c = math.cos(2.0 * math.pi * k / n)
    s = sign * math.sin(2.0 * math.pi * k / n)
    return (real * c - imag * s, real * s + imag * c)


def short_fft(z, sign):
    n = len(z)
    if n == 1:
        return z
    even = short_fft(z[0::2], sign)
    odd = short_fft(z[1::2], sign)
    low, high = [], []
    for k in range(n // 2):
        t = turned(odd[k], k, n, sign)
        low.append((even[k][0] + t[0], even[k][1] + t[1]))
        high.append((even[k][0] - t[0], even[k][1] - t[1]))
    return low + high


@functools.lru_cache(None)
def tables(ncols, nrows, lines):
    radix = ncols // LANES
    quarter = nrows // 4
    b = np.arange(LANES)
    angle = 2.0 * np.pi * (np.outer(b, b) % LANES) / LANES
    c, s = np.cos(angle), np.sin(angle)
    order = np.concatenate(
        [p * LANES + h * lines + np.arange(lines) for h in range(LANES // lines) for p in (0, 1)]
    )
    to_grid = np.block([[c, s], [-s, c]])[:, order] / math.sqrt(ncols)
    to_wave = np.block([[c, -s], [s, c]])[order, :] / math.sqrt(ncols) / 2.0
    q = np.arange(quarter)
    angle = 2.0 * np.pi * (np.outer(q, q) % quarter) / quarter
    span = np.concatenate([np.cos(angle), -np.sin(angle)], 1) * (2.0 / math.sqrt(nrows))
    angle = 2.0 * np.pi * np.outer(q, np.arange(4)) / nrows
    span_turn = np.concatenate([np.cos(angle), np.sin(angle)], 1)
    angle = 2.0 * np.pi * np.outer(np.arange(radix), b) / ncols
    line_turn = np.concatenate([np.cos(angle), np.sin(angle)], 0)
    return [np.asarray(t, np.float32) for t in (to_grid, to_wave, span, span_turn, line_turn)]


PLANE = 4
NEAR = 1
field_batches = ((0, 2), (2, 2), (4, 1))
back_batches = ((0, 1), (1, 2))


def kernel(
    groups, kept,
    vel_hbm, mask_hbm, to_grid_hbm, to_wave_hbm, span_hbm, span_turn_hbm, line_turn_hbm, kx_hbm,
    out, div,
    vel, mask, to_grid, to_wave, span, span_turn, line_turn, kx_ref,
    send, recv, vel_other, g_other, q_send, q_recv, w_other, grid,
    load_sem, send_sem, recv_sem, q_send_sem, q_recv_sem, pair_sem, pair_recv_sem, ready,
    hop, hop_sem, hop_recv_sem, pass_sem,
):
    me = lax.axis_index("pa")
    side = lax.axis_index("gz")
    partner = {"gz": 1 - side}
    kyl = vel.shape[3]
    ncols = vel.shape[4]
    lines = ncols // groups
    half = kyl * groups
    nrows = 2 * half
    quarter = half // 2
    radix = ncols // LANES
    dz = jnp.where(side == 0, 0.5, -0.5).astype(jnp.float32)

    depth = groups // PLANE
    diameter = depth + 1
    layer = me // PLANE
    column = lax.rem(me, PLANE)
    flipped = [column]
    for step in (1, 2):
        flipped += [f + step - 2 * step * lax.rem(f // step, 2) for f in flipped]
    reach = sorted(range(1 - depth, depth), key=lambda d: (-abs(d), -d))

    def columns_within(shift, low, high):
        return [c for c in range(PLANE) if low <= abs(shift) + c.bit_count() <= high]

    def each_peer(low, high, act):
        for shift in reach:
            chosen = columns_within(shift, low, high)
            if not chosen:
                continue

            def visit(shift=shift, chosen=chosen):
                for c in chosen:
                    act((layer + shift) * PLANE + flipped[c])

            if shift == 0:
                visit()
            else:
                pl.when((layer + shift >= 0) & (layer + shift < depth))(visit)

    def peers(low, high):
        total = 0
        for shift in reach:
            count = len(columns_within(shift, low, high))
            inside = (layer + shift >= 0) & (layer + shift < depth)
            total = total + jnp.where(inside, count, 0)
        return total

    barrier = pltpu.get_barrier_semaphore()
    each_peer(1, NEAR, lambda d: pl.semaphore_signal(barrier, inc=1, device_id={"pa": d}))
    pl.semaphore_signal(barrier, inc=1, device_id=partner)

    loads = {}
    for index, (name, src, dst) in enumerate(
        (
            ("v", vel_hbm.at[1], vel.at[1]),
            ("to_grid", to_grid_hbm, to_grid),
            ("line_turn", line_turn_hbm, line_turn),
            ("u", vel_hbm.at[0], vel.at[0]),
            ("w", vel_hbm.at[2], vel.at[2]),
            ("kx", kx_hbm, kx_ref),
            ("span", span_hbm, span),
            ("span_turn", span_turn_hbm, span_turn),
            ("to_wave", to_wave_hbm, to_wave),
            ("mask", mask_hbm, mask),
        )
    ):
        loads[name] = pltpu.make_async_copy(src, dst, load_sem.at[index])
        loads[name].start()

    own_n = me * kyl + lax.broadcasted_iota(jnp.int32, (kyl, LANES), 0)
    ky_own = 2.0 * math.pi / nrows * own_n.astype(jnp.float32)
    weight = jnp.where(own_n == 0, 0.5, 1.0).astype(jnp.float32)
    loads["v"].wait()
    loads["to_grid"].wait()
    loads["line_turn"].wait()
    grid_w = split(to_grid[...])

    def block(ref, a):
        return ref[:, a * LANES : (a + 1) * LANES]

    def kx_at(a):
        return jnp.broadcast_to(kx_ref[:, a * LANES : (a + 1) * LANES], (kyl, LANES))

    def spec(comp, a):
        at = slice(a * LANES, (a + 1) * LANES)
        return (vel[comp, 0, 0, :, at], vel[comp, 0, 1, :, at])

    def x_forward(slot, z):
        z = [(r * weight, i * weight) for r, i in z]
        lhs = []
        for c, (r, i) in enumerate(short_fft(z, 1.0)):
            if c > 0:
                tc = jnp.broadcast_to(line_turn[c : c + 1, :], (kyl, LANES))
                ts = jnp.broadcast_to(line_turn[radix + c : radix + c + 1, :], (kyl, LANES))
                r, i = r * tc - i * ts, r * ts + i * tc
            lhs.append(jnp.concatenate([r, i], 1))
        res = dot3(split(jnp.concatenate(lhs, 0)), grid_w)
        for c in range(radix):
            rows = res[c * kyl : (c + 1) * kyl]
            send[2 * c, slot] = rows[:, :LANES]
            send[2 * c + 1, slot] = rows[:, LANES:]

    def batch_copy(batch, dest, source):
        slots = pl.ds(*field_batches[batch])
        return pltpu.make_async_remote_copy(
            src_ref=send.at[dest, slots],
            dst_ref=recv.at[source, slots],
            send_sem=send_sem.at[batch, dest],
            recv_sem=recv_sem.at[batch, source],
            device_id={"pa": dest},
        )

    def send_batch(batch):
        @pl.loop(1, groups)
        def _(k):
            batch_copy(batch, lax.rem(me + k, groups), me).start()

        keep_own(batch)

    def keep_own(batch):
        first_slot, count = field_batches[batch]
        for slot in range(first_slot, first_slot + count):
            recv[me, slot] = send[me, slot]

    def wait_batch(batch):
        @pl.loop(1, groups)
        def _(k):
            source = lax.rem(me + groups - k, groups)

            @pl.when((source != mate) | jnp.logical_not(middle) | (batch > 0))
            def _():
                batch_copy(batch, source, source).wait_recv()

    def pair_copy(index, src, dst):
        return pltpu.make_async_remote_copy(
            src_ref=src,
            dst_ref=dst,
            send_sem=pair_sem.at[index],
            recv_sem=pair_recv_sem.at[index],
            device_id=partner,
        )

    x_forward(0, [spec(1, a) for a in range(radix)])
    pl.semaphore_wait(barrier, peers(1, NEAR) + 1)

    half_depth = depth // 2
    upper = layer >= half_depth
    middle = (layer == half_depth) | (layer == half_depth - 1)
    mate = jnp.where(upper, me - PLANE, me + PLANE)
    own_half = jnp.where(upper, groups // 2, 0)
    other_half = groups // 2 - own_half
    lead = pl.ds(*field_batches[0])

    def hop_copy(index, slot):
        return pltpu.make_async_remote_copy(
            src_ref=send.at[pl.ds(other_half + index * PLANE, PLANE), slot],
            dst_ref=hop.at[index, :, slot],
            send_sem=hop_sem.at[index, slot],
            recv_sem=hop_recv_sem.at[index, slot],
            device_id={"pa": mate},
        )

    def send_hops(slot):
        @pl.when(middle)
        def _():
            for index in range(half_depth):
                hop_copy(index, slot).start()

    def pass_copy(index, c):
        return pltpu.make_async_remote_copy(
            src_ref=hop.at[index, c],
            dst_ref=recv.at[mate, lead],
            send_sem=pass_sem.at[index, c],
            recv_sem=recv_sem.at[0, mate],
            device_id={"pa": own_half + index * PLANE + c},
        )

    def each_pass(index, act):
        for c in range(PLANE):

            @pl.when(own_half + index * PLANE + c != me)
            def _():
                act(pass_copy(index, c))

    def pass_on():
        @pl.when(middle)
        def _():
            for index in range(half_depth):
                for slot in range(field_batches[0][1]):
                    hop_copy(index, slot).wait_recv()
                each_pass(index, lambda copy: copy.start())
                for c in range(PLANE):

                    @pl.when(own_half + index * PLANE + c == me)
                    def _():
                        recv[mate, lead] = hop[index, c]

    def direct(dest):
        return jnp.logical_not(middle & ((dest >= groups // 2) != upper))

    steps = []
    known = NEAR
    while known < diameter:
        steps.append(min(known, diameter - known))
        known += steps[-1]

    def tell(index):
        if index < len(steps):
            each_peer(
                1,
                steps[index],
                lambda d: pl.semaphore_signal(ready.at[index], inc=1, device_id={"pa": d}),
            )

    def hear(index):
        if index < len(steps):
            pl.semaphore_wait(ready.at[index], peers(1, steps[index]))
            tell(index + 1)

    send_hops(0)
    tell(0)
    loads["u"].wait()
    x_forward(1, [spec(0, a) for a in range(radix)])
    send_hops(1)
    loads["w"].wait()
    loads["kx"].wait()
    keep_own(0)
    vel_copies = [pair_copy(f, vel.at[f, 0], vel_other.at[f]) for f in range(3)]
    for copy in vel_copies:
        copy.start()
    x_forward(2, [spec(2, a) for a in range(radix)])
    hear(0)
    vel_copies[0].wait_recv()
    swirl = []
    for a in range(radix):
        w, kx = spec(2, a), kx_at(a)
        at = slice(a * LANES, (a + 1) * LANES)
        swirl.append((dz * vel_other[0, 0, :, at] + kx * w[1], dz * vel_other[0, 1, :, at] - kx * w[0]))
    x_forward(3, swirl)
    for index in range(1, len(steps)):
        hear(index)

    @pl.loop(1, groups)
    def _(k):
        dest = lax.rem(me + k, groups)

        @pl.when(direct(dest))
        def _():
            batch_copy(0, dest, me).start()

    send_batch(1)
    swirl = []
    for a in range(radix):
        v, u, kx = spec(1, a), spec(0, a), kx_at(a)
        swirl.append((ky_own * u[1] - kx * v[1], kx * v[0] - ky_own * u[0]))
    x_forward(4, swirl)
    send_batch(2)

    vel_copies[1].wait_recv()
    vel_copies[2].wait_recv()
    ky_wide = ky_own[:, :1]
    square = kx_ref[...] * kx_ref[...] + ky_wide * ky_wide
    for f in range(3):
        for part in range(2):
            own = vel[f, 0, part]
            viscous = vel_other[f, part] - 2.0 * own - square * own
            out[f, 0, part] = own + time_step * viscosity * viscous

    loads["span"].wait()
    loads["span_turn"].wait()
    span_w = split(span[...])
    lane = lax.broadcasted_iota(jnp.int32, (half, LANES), 1)
    first = lane < lines
    all_n = lax.broadcasted_iota(jnp.int32, (half, LANES), 0)
    ky_all = 2.0 * math.pi / nrows * all_n.astype(jnp.float32)
    ky_all = jnp.where(first, -ky_all, ky_all)

    def swap(value):
        return pltpu.roll(value, lines, 1)

    def turn(t):
        c = jnp.broadcast_to(span_turn[:, t : t + 1], (quarter, LANES))
        s = jnp.broadcast_to(span_turn[:, 4 + t : 5 + t], (quarter, LANES))
        return c, s

    def field(slot):
        return recv[:, slot].reshape(half, LANES)

    def y_forward(pair, one, two):
        real = jnp.where(first, one, swap(two))
        imag = jnp.where(first, swap(one), two)
        rl, rh, il, ih = real[:quarter], real[quarter:], imag[:quarter], imag[quarter:]
        columns = []
        for t, (r, i) in enumerate(
            [(rl + rh, il + ih), (rl - ih, il + rh), (rl - rh, il - ih), (rl + ih, il - rh)]
        ):
            if t > 0:
                c, s = turn(t)
                r, i = r * c - i * s, r * s + i * c
            columns.append(jnp.concatenate([r, i], 0))
        res = dot3(span_w, split(jnp.concatenate(columns, 1)))
        for t in range(4):
            grid[pair, t] = res[:, t * LANES : (t + 1) * LANES]

    back_w = span[...]
    back_w = split(jnp.concatenate([back_w[:, :quarter], back_w[:, quarter:]], 0))
    lo = lax.broadcasted_iota(jnp.int32, (quarter, LANES), 1) < lines

    def q_copy(batch, dest, source):
        slots = pl.ds(*back_batches[batch])
        return pltpu.make_async_remote_copy(
            src_ref=q_send.at[dest, slots],
            dst_ref=q_recv.at[source, slots],
            send_sem=q_send_sem.at[batch, dest],
            recv_sem=q_recv_sem.at[batch, source],
            device_id={"pa": dest},
        )

    def q_start(batch):
        @pl.loop(1, groups)
        def _(k):
            dest = lax.rem(me + k, groups)

            @pl.when(dest < kept)
            def _():
                q_copy(batch, dest, me).start()

        first_slot, count = back_batches[batch]
        for slot in range(first_slot, first_slot + count):
            q_recv[me, slot] = q_send[me, slot]

    def q_wait(batch, first_source, last_source):
        @pl.loop(first_source, last_source)
        def _(source):
            @pl.when(source != me)
            def _():
                q_copy(batch, source, source).wait_recv()

    def y_back(columns, comps):
        res = dot3(back_w, split(jnp.concatenate(columns, 1)))
        sums = []
        for t in range(4):
            r = res[:quarter, t * LANES : (t + 1) * LANES]
            i = res[quarter:, t * LANES : (t + 1) * LANES]
            if t > 0:
                c, s = turn(t)
                r, i = r * c + i * s, i * c - r * s
            sums.append((r, i))
        (r0, i0), (r1, i1), (r2, i2), (r3, i3) = sums
        low = (r0 + r1 + r2 + r3, i0 + i1 + i2 + i3)
        high = (r0 - r2 + (i1 - i3), i0 - i2 - (r1 - r3))
        for base, (r, i), count in (
            (0, low, quarter // kyl),
            (quarter // kyl, high, kept - quarter // kyl),
        ):
            rolled_i, rolled_r = swap(i), swap(r)
            packed = [jnp.where(lo, r, rolled_i), jnp.where(lo, rolled_r, i)]
            for comp, value in zip(comps, packed):
                q_send[base : base + count, comp] = value[: count * kyl].reshape(count, kyl, LANES)

    pass_on()
    wait_batch(0)
    v_copy = pair_copy(3, recv.at[:, 0], g_other)
    v_copy.start()
    y_forward(0, field(1), field(0))
    wait_batch(1)
    v_copy.wait_recv()
    swirl_x = ky_all * swap(field(2)) - dz * g_other[...].reshape(half, LANES)
    y_forward(1, field(3), swirl_x)
    columns = []
    for t in range(4):
        product = grid[0, t] * grid[1, t]
        columns.append(product - swap(product))
    y_back(columns, (0,))
    q_start(0)
    wait_batch(2)
    y_forward(2, field(2), field(4))
    columns = []
    for t in range(4):
        speed, swirls, mixed = grid[0, t], grid[1, t], grid[2, t]
        x_part = swap(speed * mixed) - mixed * swirls
        y_part = mixed * swap(swirls) - speed * swap(mixed)
        columns.append(jnp.where(lo, x_part, swap(y_part)))
    y_back(columns, (1, 2))
    q_start(1)

    loads["to_wave"].wait()
    loads["mask"].wait()
    wave_w = split(to_wave[...])

    def x_lines(slot, residues):
        rows = [
            jnp.concatenate([q_recv[2 * c, slot], q_recv[2 * c + 1, slot]], 1) for c in residues
        ]
        res = dot3(split(jnp.concatenate(rows, 0)), wave_w)
        return [res[j * kyl : (j + 1) * kyl] for j in range(len(residues))]

    def x_back(comp, lines_of):
        z = []
        for c in range(radix):
            r = lines_of[c][:, :LANES]
            i = lines_of[c][:, LANES:]
            if c > 0:
                tc = jnp.broadcast_to(line_turn[c : c + 1, :], (kyl, LANES))
                ts = jnp.broadcast_to(line_turn[radix + c : radix + c + 1, :], (kyl, LANES))
                r, i = r * tc + i * ts, i * tc - r * ts
            z.append((r, i))
        for a, values in enumerate(short_fft(z, -1.0)):
            at = slice(a * LANES, (a + 1) * LANES)
            gain = time_step * mask[:, at].astype(jnp.float32)
            for part in range(2):
                out[comp, 0, part, :, at] = out[comp, 0, part, :, at] + gain * values[part]

    @pl.when(me < kept)
    def _():
        q_wait(0, 0, groups)
        x_back(2, x_lines(0, range(radix)))

    w_copy = pair_copy(4, out.at[2, 0], w_other)
    w_copy.start()

    for copy in vel_copies + [v_copy, w_copy]:
        copy.wait_send()

    @pl.when(middle)
    def _():
        for index in range(half_depth):
            for slot in range(field_batches[0][1]):
                hop_copy(index, slot).wait_send()
            each_pass(index, lambda copy: copy.wait_send())

    for batch in range(len(field_batches)):

        @pl.loop(1, groups)
        def _(k):
            dest = lax.rem(me + k, groups)

            @pl.when(direct(dest) | (batch > 0))
            def _():
                batch_copy(batch, dest, me).wait_send()

    for batch in range(len(back_batches)):

        @pl.loop(1, groups)
        def _(k):
            dest = lax.rem(me + k, groups)

            @pl.when(dest < kept)
            def _():
                q_copy(batch, dest, me).wait_send()

    w_copy.wait_recv()

    @pl.when(me < kept)
    def _():
        half_radix = radix // 2
        q_wait(1, 0, groups // 2)
        near = [x_lines(slot, range(half_radix)) for slot in (1, 2)]
        q_wait(1, groups // 2, groups)
        for slot in (1, 2):
            x_back(slot - 1, near[slot - 1] + x_lines(slot, range(half_radix, radix)))

    kx_all = kx_ref[...]
    for part, sign in ((0, -1.0), (1, 1.0)):
        u_next = out[0, 0, 1 - part]
        v_next = out[1, 0, 1 - part]
        div[0, part] = dz * w_other[part] + sign * (kx_all * u_next + ky_wide * v_next)


def store_kernel(next_ref, div_ref, next_out, div_out, sem):
    copies = [
        pltpu.make_async_copy(next_ref.at[f, 0, p], next_out.at[f, 0, p], sem.at[2 * f + p])
        for f in range(3)
        for p in range(2)
    ]
    copies += [
        pltpu.make_async_copy(div_ref.at[0, p], div_out.at[0, p], sem.at[6 + p]) for p in range(2)
    ]
    for copy in copies:
        copy.start()
    for copy in copies:
        copy.wait()


def in_one_kernel(velocity, mode_mask):
    groups = lax.axis_size("pa")
    kyl = velocity.shape[3]
    ncols = velocity.shape[4]
    lines = ncols // groups
    half = kyl * groups
    nrows = 2 * half
    kept = -(-(nrows // 3) // kyl)
    signed = np.where(np.arange(ncols) < ncols // 2, np.arange(ncols), np.arange(ncols) - ncols)
    kx = (np.float32(2.0 * math.pi / ncols) * signed.astype(np.float32))[None, :]
    operands = [velocity, mode_mask] + [jnp.asarray(t) for t in tables(ncols, nrows, lines)]
    operands.append(jnp.asarray(kx))
    f32 = jnp.float32
    halves = groups // PLANE // 2
    hbm = pl.BlockSpec(memory_space=pltpu.HBM)
    whole = pl.BlockSpec(memory_space=pl.ANY)
    vmem = pl.BlockSpec(memory_space=pltpu.VMEM)
    dma = pltpu.SemaphoreType.DMA
    shapes = (
        jax.ShapeDtypeStruct(velocity.shape, f32),
        jax.ShapeDtypeStruct(velocity.shape[1:], f32),
    )
    following, divergence = pl.pallas_call(
        functools.partial(kernel, groups, kept),
        out_shape=shapes,
        in_specs=[hbm] * len(operands),
        out_specs=(vmem, vmem),
        scratch_shapes=[pltpu.VMEM(t.shape, t.dtype) for t in operands]
        + [
            pltpu.VMEM((groups, 5, kyl, LANES), f32),
            pltpu.VMEM((groups, 5, kyl, LANES), f32),
            pltpu.VMEM((3, 2, kyl, ncols), f32),
            pltpu.VMEM((groups, kyl, LANES), f32),
            pltpu.VMEM((groups, 3, kyl, LANES), f32),
            pltpu.VMEM((groups, 3, kyl, LANES), f32),
            pltpu.VMEM((2, kyl, ncols), f32),
            pltpu.VMEM((3, 4, half // 2, LANES), f32),
            dma((10,)),
            dma((len(field_batches), groups)),
            dma((len(field_batches), groups)),
            dma((len(back_batches), groups)),
            dma((len(back_batches), groups)),
            dma((5,)),
            dma((5,)),
            pltpu.SemaphoreType.REGULAR((groups,)),
            pltpu.VMEM((halves, PLANE, field_batches[0][1], kyl, LANES), f32),
            dma((halves, field_batches[0][1])),
            dma((halves, field_batches[0][1])),
            dma((halves, PLANE)),
        ],
        compiler_params=pltpu.CompilerParams(collective_id=0, has_side_effects=True, vmem_limit_bytes=32 * 2**20),
    )(*[pltpu.with_memory_space_constraint(x, pltpu.HBM) for x in operands])
    return pl.pallas_call(
        store_kernel,
        out_shape=shapes,
        in_specs=[whole, whole],
        out_specs=(hbm, hbm),
        scratch_shapes=[dma((8,))],
        compiler_params=pltpu.CompilerParams(vmem_limit_bytes=2**20),
    )(following, divergence)


def on_device(velocity, mode_mask):
    groups = lax.axis_size("pa")
    kyl = velocity.shape[3]
    ncols = velocity.shape[4]
    fits = (
        lax.axis_size("gz") == 2
        and velocity.shape[1] == 1
        and kyl % 8 == 0
        and groups % (2 * PLANE) == 0
        and 2 * (ncols // groups) == LANES
        and (kyl * groups // 2) % LANES == 0
        and ncols % LANES == 0
        and nrows_cover(kyl * groups)
    )
    return in_one_kernel(velocity, mode_mask) if fits else by_steps(velocity, mode_mask)


def nrows_cover(half):
    return 2 * half // 3 > half // 2


def solution(mesh):
    placed = (P(None, "gz", None, "pa", None), P("pa", None))
    return jax.shard_map(
        on_device,
        mesh=mesh,
        in_specs=placed,
        out_specs=(P(None, "gz", None, "pa", None), P("gz", None, "pa", None)),
        check_vma=False,
    )
```
